8 devices in a mesh: batch: 1 (over z), col: 2 (over y), row: 4 (over x, core).
Axes of the slice: x: 2, y: 2, z: 1, core: 2. Of those that a mesh axis runs over, the one named last changes fastest.
Arguments:
- mat_blocks: float32 [8192, 256, 64], P(('batch', 'row'), 'col')
Outputs:
- output 1: float32 [8192, 256, 64], P(('batch', 'row'), 'col')
- output 2: float32 [256], P('batch')
- output 3: float32 [4, 64, 64], P('batch')
All inputs are finite; a program needn't handle non-finite values.
Results may differ from the reference program's by a relative error of at most 0.001.
Values sent between devices are 32-bit elements.
A program may use at most 1 GiB of HBM per device.

```python
import math
import jax
import jax.numpy as jnp
from jax import lax

MATRIX_ROWS = 8192
MATRIX_COLS = 16384
BLOCK_COLS = 64
PANELS = 4
COL_PROCS = 2
PANEL_COLS = PANELS * BLOCK_COLS
TOTAL_BLOCKS = MATRIX_COLS // BLOCK_COLS
LOCAL_BLOCKS = TOTAL_BLOCKS // COL_PROCS
HIGHEST = lax.Precision.HIGHEST


def mat_dot(left_mat, right_mat):
    return jnp.dot(left_mat, right_mat, precision=HIGHEST, preferred_element_type=jnp.float32)


def to_stored(glob_mat):
    split_mat = glob_mat.reshape(MATRIX_ROWS, LOCAL_BLOCKS, COL_PROCS, BLOCK_COLS)
    return split_mat.transpose(0, 2, 1, 3).reshape(MATRIX_ROWS, TOTAL_BLOCKS, BLOCK_COLS)


def to_global(stored_mat):
    split_mat = stored_mat.reshape(MATRIX_ROWS, COL_PROCS, LOCAL_BLOCKS, BLOCK_COLS)
    return split_mat.transpose(0, 2, 1, 3).reshape(MATRIX_ROWS, MATRIX_COLS)


def setup_inputs(seed: int = 0, part: int = 0) -> dict:
    base_key = jax.random.fold_in(jax.random.key(seed), part)
    key_gauss, key_left, key_right, key_sign = jax.random.split(base_key, 4)
    gauss_part = jax.random.normal(key_gauss, (MATRIX_ROWS, MATRIX_COLS), jnp.float32)
    low_left = jax.random.normal(key_left, (MATRIX_ROWS, 4), jnp.float32)
    low_right = 0.35 * jax.random.normal(key_right, (4, MATRIX_COLS), jnp.float32)
    pivot_sign = 2.0 * jax.random.randint(key_sign, (PANEL_COLS,), 0, 2).astype(jnp.float32) - 1.0
    dense_mat = gauss_part + mat_dot(low_left, low_right)
    diag_ids = jnp.arange(PANEL_COLS)
    dense_mat = dense_mat.at[diag_ids, diag_ids].add(1.2 * math.sqrt(MATRIX_ROWS) * pivot_sign)
    return {'mat_blocks': to_stored(dense_mat)}


def factor_panel(panel_in, pivot_base):
    row_ids = jnp.arange(MATRIX_ROWS)
    col_ids = jnp.arange(BLOCK_COLS)

    def column_step(col_idx, loop_state):
        panel_work, tau_vec = loop_state
        pivot_row = pivot_base + col_idx
        column = lax.dynamic_index_in_dim(panel_work, col_idx, axis=1, keepdims=False)
        alpha_val = lax.dynamic_index_in_dim(column, pivot_row, keepdims=False)
        sub_col = jnp.where(row_ids > pivot_row, column, 0.0)
        norm_val = jnp.sqrt(alpha_val * alpha_val + jnp.sum(sub_col * sub_col))
        beta_val = jnp.where(alpha_val >= 0.0, -norm_val, norm_val)
        tau_val = (beta_val - alpha_val) / beta_val
        refl_vec = sub_col / (alpha_val - beta_val) + jnp.where(row_ids == pivot_row, 1.0, 0.0)
        refl_dot = mat_dot(refl_vec[None, :], panel_work)[0]
        refl_dot = jnp.where(col_ids > col_idx, refl_dot, 0.0)
        new_col = jnp.where(row_ids < pivot_row, column, jnp.where(row_ids == pivot_row, beta_val, refl_vec))
        panel_work = panel_work - tau_val * refl_vec[:, None] * refl_dot[None, :]
        panel_work = jnp.where(col_ids[None, :] == col_idx, new_col[:, None], panel_work)
        tau_vec = jnp.where(col_ids == col_idx, tau_val, tau_vec)
        return panel_work, tau_vec

    return lax.fori_loop(0, BLOCK_COLS, column_step, (panel_in, jnp.zeros((BLOCK_COLS,), jnp.float32)))


def form_tfactor(refl_mat, tau_vec):
    gram_mat = mat_dot(refl_mat.T, refl_mat)
    col_ids = jnp.arange(BLOCK_COLS)

    def tcol_step(col_idx, t_factor):
        gram_col = lax.dynamic_index_in_dim(gram_mat, col_idx, axis=1, keepdims=False)
        tau_val = lax.dynamic_index_in_dim(tau_vec, col_idx, keepdims=False)
        gram_col = jnp.where(col_ids < col_idx, gram_col, 0.0)
        new_col = -tau_val * mat_dot(t_factor, gram_col[:, None])[:, 0]
        new_col = jnp.where(col_ids == col_idx, tau_val, new_col)
        return jnp.where(col_ids[None, :] == col_idx, new_col[:, None], t_factor)

    return lax.fori_loop(0, BLOCK_COLS, tcol_step, jnp.zeros((BLOCK_COLS, BLOCK_COLS), jnp.float32))


def reference(mat_blocks):
    glob_mat = to_global(mat_blocks)
    row_ids = jnp.arange(MATRIX_ROWS)
    col_ids = jnp.arange(BLOCK_COLS)
    tau_list = []
    tfac_list = []
    for panel_idx in range(PANELS):
        col_start = panel_idx * BLOCK_COLS
        col_end = col_start + BLOCK_COLS
        panel_out, tau_vec = factor_panel(glob_mat[:, col_start:col_end], col_start)
        pivot_ids = col_start + col_ids
        refl_mat = jnp.where(row_ids[:, None] > pivot_ids[None, :], panel_out, jnp.where(row_ids[:, None] == pivot_ids[None, :], 1.0, 0.0))
        t_factor = form_tfactor(refl_mat, tau_vec)
        trail_mat = glob_mat[:, col_end:]
        w_mat = mat_dot(t_factor.T, mat_dot(refl_mat.T, trail_mat))
        trail_mat = trail_mat - mat_dot(refl_mat, w_mat)
        glob_mat = jnp.concatenate([glob_mat[:, :col_start], panel_out, trail_mat], axis=1)
        tau_list.append(tau_vec)
        tfac_list.append(t_factor)
    return to_stored(glob_mat), jnp.concatenate(tau_list), jnp.stack(tfac_list)
```

```python
import jax
import jax.numpy as jnp
from jax import lax
from jax.experimental import pallas as pl
from jax.experimental.pallas import tpu as pltpu
from jax.sharding import PartitionSpec as P

NB = 64
LANES = 128
PANELS = 4
WIDTH = NB * PANELS
HIGHEST = lax.Precision.HIGHEST


def split3(x):
    high = x.astype(jnp.bfloat16)
    rest = x - high.astype(jnp.float32)
    mid = rest.astype(jnp.bfloat16)
    low = (rest - mid.astype(jnp.float32)).astype(jnp.bfloat16)
    return high, mid, low


def small_dot(a, b):
    return jnp.dot(a, b, precision=HIGHEST, preferred_element_type=jnp.float32)


def factor_panel(panel, src_ref, out_ref, vs_ref, st_ref, h_ref):
    n_tiles = src_ref.shape[0]
    base = panel * NB
    lane = lax.broadcasted_iota(jnp.int32, (8, LANES), 1)
    sub = lax.broadcasted_iota(jnp.int32, (8, LANES), 0)
    groups = NB // 8
    zero = jnp.zeros((8, LANES), jnp.float32)

    def tile(g, t):
        return (t, pl.ds(base + 8 * g, 8), slice(None))

    def splat(v):
        return jnp.broadcast_to(jnp.sum(v, axis=1, keepdims=True), (8, LANES))

    def row(ref, j, t):
        return ref[t, pl.ds(base + j, 8, stride=0), :]

    def finish(acc, piv, accn, alf):
        return [splat(a) for a in acc], [splat(a) for a in piv], splat(accn), splat(alf)

    def start():
        acc = [zero] * groups
        piv = [zero] * groups
        accn = zero
        alf = zero
        for t in range(n_tiles):
            x = row(src_ref, 0, t)
            if t < 2:
                rid = lane + t * LANES
                alf = alf + jnp.where(rid == base, x, 0.0)
                x = jnp.where(rid > base, x, 0.0)
            accn = accn + x * x
            for g in range(groups):
                a = src_ref[tile(g, t)]
                if src_ref is not out_ref:
                    out_ref[tile(g, t)] = a
                if t < 2:
                    piv[g] = piv[g] + jnp.where(rid == base, a, 0.0)
                acc[g] = acc[g] + x * a
        return finish(acc, piv, accn, alf)

    carry = start()
    for g0 in range(groups):
        n_g = groups - g0

        def step(s, carry, g0=g0, n_g=n_g):
            (dots, pivs, norm2, alpha), coef = carry
            j = g0 * 8 + s
            k = base + j
            norm = jnp.sqrt(alpha * alpha + norm2)
            beta = jnp.where(alpha >= 0.0, -norm, norm)
            tau = (beta - alpha) / beta
            scale = 1.0 / (alpha - beta)
            coef = [jnp.where(sub == s, new, old) for new, old in zip((tau, scale, beta), coef)]
            hs, fs = [], []
            for i in range(n_g):
                f = tau * (scale * dots[i] + pivs[i])
                if i == 0:
                    f = jnp.where(sub > s, f, 0.0)
                h = f * scale
                h_ref[pl.ds(8 * (g0 + i), 8), :] = h
                h_ref[pl.ds(NB + 8 * (g0 + i), 8), :] = f
                hs.append(h)
                fs.append(f)
            j1 = jnp.minimum(j + 1, NB - 1)
            k1 = k + 1
            h1 = h_ref[pl.ds(j1, 8, stride=0), :]
            f1 = h_ref[pl.ds(NB + j1, 8, stride=0), :]
            acc = [zero] * n_g
            piv = [zero] * n_g
            accn = zero
            alf = zero
            for t in range(n_tiles):
                x = row(out_ref, j, t)
                x1 = row(out_ref, j1, t)
                if t < 2:
                    rid = lane + t * LANES
                    xm = jnp.where(rid > k, x, 0.0)
                    pm = jnp.where(rid == k, 1.0, 0.0)
                    x1 = x1 - h1 * xm - f1 * pm
                    alf = alf + jnp.where(rid == k1, x1, 0.0)
                    x1 = jnp.where(rid > k1, x1, 0.0)
                else:
                    x1 = x1 - h1 * x
                accn = accn + x1 * x1
                for i in range(n_g):
                    a = out_ref[tile(g0 + i, t)]
                    if t < 2:
                        a = a - hs[i] * xm - fs[i] * pm
                        piv[i] = piv[i] + jnp.where(rid == k1, a, 0.0)
                    else:
                        a = a - hs[i] * x
                    out_ref[tile(g0 + i, t)] = a
                    acc[i] = acc[i] + x1 * a
            return finish(acc, piv, accn, alf), coef

        carry, coef = lax.fori_loop(0, 8, step, (carry, [zero] * 3))
        for i in range(3):
            st_ref[i, pl.ds(8 * g0, 8), :] = coef[i]
        dots, pivs, norm2, alpha = carry
        carry = (dots[1:], pivs[1:], norm2, alpha)

    lane16 = lax.broadcasted_iota(jnp.int32, (16, LANES), 1)
    sub16 = lax.broadcasted_iota(jnp.int32, (16, LANES), 0)
    for g in range(groups // 2):
        scale = st_ref[1, pl.ds(16 * g, 16), :]
        beta = st_ref[2, pl.ds(16 * g, 16), :]
        kk = base + 16 * g + sub16
        place = pl.ds(base + 16 * g, 16)
        for t in range(n_tiles):
            a = out_ref[t, place, :]
            v = a * scale
            full = v
            if t < 2:
                rid = lane16 + t * LANES
                full = jnp.where(rid > kk, v, jnp.where(rid == kk, beta, a))
                v = jnp.where(rid > kk, v, jnp.where(rid == kk, 1.0, 0.0))
            out_ref[t, place, :] = full
            for i, part in enumerate(split3(v)):
                vs_ref[i, t, place, :] = part


def panel_dots(load_lhs, rows, panel, vs_ref, acc_ref, n_tiles):
    step_tiles = 8
    acc_ref[pl.ds(0, rows), :] = jnp.zeros((rows, NB), jnp.float32)

    def body(chunk, _):
        parts = [load_lhs(chunk * step_tiles + i) for i in range(step_tiles)]
        lhs = jnp.concatenate([jnp.concatenate([p[s] for p in parts], axis=1) for s in range(3)], axis=0)
        rhs = jnp.concatenate(
            [
                jnp.concatenate(
                    [vs_ref[s, chunk * step_tiles + i, pl.ds(panel * NB, NB), :] for i in range(step_tiles)], axis=1
                )
                for s in range(3)
            ],
            axis=0,
        )
        prod = lax.dot_general(lhs, rhs, (((1,), (1,)), ((), ())), preferred_element_type=jnp.float32)
        top, mid, low = prod[:rows], prod[rows : 2 * rows], prod[2 * rows :]
        small = (top[:, 2 * NB :] + low[:, :NB]) + mid[:, NB : 2 * NB]
        acc_ref[pl.ds(0, rows), :] += (small + (top[:, NB : 2 * NB] + mid[:, :NB])) + top[:, :NB]
        return 0

    lax.fori_loop(0, n_tiles // step_tiles, body, 0)
    return acc_ref[pl.ds(0, rows), :]


def t_from_gram(gram, tau_rows):
    ii = lax.broadcasted_iota(jnp.int32, (NB, NB), 0)
    jj = lax.broadcasted_iota(jnp.int32, (NB, NB), 1)
    eye = jnp.where(ii == jj, 1.0, 0.0)
    power = jnp.where(jj > ii, -tau_rows * gram, 0.0)
    inv = eye + power
    for _ in range(5):
        power = small_dot(power, power)
        inv = inv + small_dot(inv, power)
    tau_cols = jnp.sum(jnp.where(ii == jj, tau_rows, 0.0), axis=0, keepdims=True)
    return inv * tau_cols


def factor_all_kernel(p_ref, out_ref, vs_ref, t_ref, tfull_ref, st_ref, h_ref, acc_ref):
    n_tiles = p_ref.shape[0]
    tfull_ref[...] = jnp.zeros_like(tfull_ref)
    for panel in range(PANELS):
        src = p_ref if panel == 0 else out_ref
        factor_panel(panel, src, out_ref, vs_ref, st_ref, h_ref)
        seen = NB * (panel + 1)
        gram = panel_dots(
            lambda t: [vs_ref[s, t, pl.ds(0, seen), :] for s in range(3)], seen, panel, vs_ref, acc_ref, n_tiles
        )
        t_mat = t_from_gram(gram[seen - NB :], st_ref[0][:, :NB])
        t_ref[panel] = t_mat
        here = pl.ds(seen - NB, NB)
        tfull_ref[here, here] = t_mat
        if panel:
            before = pl.ds(0, seen - NB)
            cross = small_dot(tfull_ref[before, before], gram[: seen - NB])
            tfull_ref[before, here] = -small_dot(cross, t_mat)
        if panel == PANELS - 1:
            break
        left = WIDTH - seen
        rest = pl.ds(seen, left)
        w_sum = panel_dots(lambda t: split3(src[t, rest, :]), left, panel, vs_ref, acc_ref, n_tiles)
        high, mid, low = split3(small_dot(w_sum, t_mat))
        lhs = jnp.concatenate([high, high, high, mid, mid, low], axis=1)

        def body(pair, _):
            tiles = (2 * pair, 2 * pair + 1)
            rhs = jnp.concatenate(
                [
                    jnp.concatenate([vs_ref[s, t, pl.ds(panel * NB, NB), :] for t in tiles], axis=1)
                    for s in (0, 1, 2, 0, 1, 0)
                ],
                axis=0,
            )
            prod = jnp.dot(lhs, rhs, preferred_element_type=jnp.float32)
            for i, t in enumerate(tiles):
                out_ref[t, rest, :] = src[t, rest, :] - prod[:, i * LANES : (i + 1) * LANES]
            return 0

        lax.fori_loop(0, n_tiles // 2, body, 0)


def factor_all(panels):
    n_tiles = panels.shape[0]
    vmem = pl.BlockSpec(memory_space=pltpu.VMEM)
    return pl.pallas_call(
        factor_all_kernel,
        out_shape=(
            jax.ShapeDtypeStruct(panels.shape, jnp.float32),
            jax.ShapeDtypeStruct((3, *panels.shape), jnp.bfloat16),
            jax.ShapeDtypeStruct((PANELS, NB, NB), jnp.float32),
            jax.ShapeDtypeStruct((WIDTH, WIDTH), jnp.float32),
        ),
        in_specs=[vmem],
        out_specs=[vmem] * 4,
        scratch_shapes=[
            pltpu.VMEM((3, NB, LANES), jnp.float32),
            pltpu.VMEM((2 * NB, LANES), jnp.float32),
            pltpu.VMEM((WIDTH, NB), jnp.float32),
        ],
        compiler_params=pltpu.CompilerParams(vmem_limit_bytes=60 * 1024 * 1024),
        name="factor_all",
    )(panels)


def solution(mesh):
    col_count = mesh.shape['col']
    block_spec = P(('batch', 'row'), 'col', None)
    own = PANELS // col_count

    def device_fn(a_local):
        local_rows, local_blocks, _ = a_local.shape
        local_tiles = local_rows // LANES
        col_rank = lax.axis_index('col')
        row_rank = lax.axis_index('row')
        share = a_local[:, :own, :].reshape(local_tiles, LANES, own, NB).transpose(2, 0, 3, 1)
        every = lax.all_gather(lax.all_gather(share, 'row'), 'col')
        panels = every.transpose(1, 3, 2, 0, 4, 5).reshape(-1, WIDTH, LANES)
        packed, _, t_factors, t_full = factor_all(panels)
        packed = lax.dynamic_slice_in_dim(packed, row_rank * local_tiles, local_tiles, 0)
        rows = row_rank * local_rows + jnp.arange(local_rows).reshape(local_tiles, 1, LANES)
        cols = jnp.arange(WIDTH).reshape(1, WIDTH, 1)
        refl = jnp.where(rows > cols, packed, jnp.where(rows == cols, 1.0, 0.0))
        refl = refl.transpose(1, 0, 2).reshape(WIDTH, local_rows)
        w_sum = lax.psum(jnp.einsum('kr,rbc->kbc', refl, a_local, precision=HIGHEST, preferred_element_type=jnp.float32), 'row')
        w_mat = jnp.einsum('kj,kbc->jbc', t_full, w_sum, precision=HIGHEST, preferred_element_type=jnp.float32)
        global_ids = jnp.arange(local_blocks) * col_count + col_rank
        w_mat = jnp.where((global_ids >= PANELS)[None, :, None], w_mat, 0.0)
        a_new = a_local - jnp.einsum('jr,jbc->rbc', refl, w_mat, precision=HIGHEST, preferred_element_type=jnp.float32)
        mine = packed.reshape(local_tiles, own, col_count, NB, LANES)
        mine = lax.dynamic_index_in_dim(mine, col_rank, 2, keepdims=False).transpose(0, 3, 1, 2).reshape(local_rows, own, NB)
        mine = jnp.pad(mine, ((0, 0), (0, local_blocks - own), (0, 0)))
        a_new = jnp.where((global_ids < PANELS)[None, :, None], mine, a_new)
        tau = jnp.diagonal(t_factors, axis1=1, axis2=2).reshape(-1)
        return a_new, tau, t_factors

    return jax.shard_map(device_fn, mesh=mesh, in_specs=(block_spec,), out_specs=(block_spec, P('batch'), P('batch', None, None)), check_vma=False)
```

```python
import jax
import jax.numpy as jnp
from jax import lax
from jax.experimental import pallas as pl
from jax.experimental.pallas import tpu as pltpu
from jax.sharding import PartitionSpec as P

NB = 64
LANES = 128
PANELS = 4
WIDTH = NB * PANELS
HIGHEST = lax.Precision.HIGHEST


def split3(x):
    high = x.astype(jnp.bfloat16)
    rest = x - high.astype(jnp.float32)
    mid = rest.astype(jnp.bfloat16)
    low = (rest - mid.astype(jnp.float32)).astype(jnp.bfloat16)
    return high, mid, low


def small_dot(a, b):
    return jnp.dot(a, b, precision=HIGHEST, preferred_element_type=jnp.float32)


def factor_panel(panel, src_ref, out_ref, vs_ref, st_ref, h_ref):
    n_tiles = src_ref.shape[0]
    base = panel * NB
    lane = lax.broadcasted_iota(jnp.int32, (8, LANES), 1)
    sub = lax.broadcasted_iota(jnp.int32, (8, LANES), 0)
    groups = NB // 8
    zero = jnp.zeros((8, LANES), jnp.float32)

    def tile(g, t):
        return (t, pl.ds(base + 8 * g, 8), slice(None))

    def splat(v):
        return jnp.broadcast_to(jnp.sum(v, axis=1, keepdims=True), (8, LANES))

    def row(ref, j, t):
        return ref[t, pl.ds(base + j, 8, stride=0), :]

    def finish(acc, piv, accn, alf):
        return [splat(a) for a in acc], [splat(a) for a in piv], splat(accn), splat(alf)

    def start():
        acc = [zero] * groups
        piv = [zero] * groups
        accn = zero
        alf = zero
        for t in range(n_tiles):
            x = row(src_ref, 0, t)
            if t < 2:
                rid = lane + t * LANES
                alf = alf + jnp.where(rid == base, x, 0.0)
                x = jnp.where(rid > base, x, 0.0)
            accn = accn + x * x
            for g in range(groups):
                a = src_ref[tile(g, t)]
                if src_ref is not out_ref:
                    out_ref[tile(g, t)] = a
                if t < 2:
                    piv[g] = piv[g] + jnp.where(rid == base, a, 0.0)
                acc[g] = acc[g] + x * a
        return finish(acc, piv, accn, alf)

    carry = start()
    for g0 in range(groups):
        n_g = groups - g0

        def step(s, carry, g0=g0, n_g=n_g):
            (dots, pivs, norm2, alpha), coef = carry
            j = g0 * 8 + s
            k = base + j
            norm = jnp.sqrt(alpha * alpha + norm2)
            beta = jnp.where(alpha >= 0.0, -norm, norm)
            tau = (beta - alpha) / beta
            scale = 1.0 / (alpha - beta)
            coef = [jnp.where(sub == s, new, old) for new, old in zip((tau, scale, beta), coef)]
            hs, fs = [], []
            for i in range(n_g):
                f = tau * (scale * dots[i] + pivs[i])
                if i == 0:
                    f = jnp.where(sub > s, f, 0.0)
                h = f * scale
                h_ref[pl.ds(8 * (g0 + i), 8), :] = h
                h_ref[pl.ds(NB + 8 * (g0 + i), 8), :] = f
                hs.append(h)
                fs.append(f)
            j1 = jnp.minimum(j + 1, NB - 1)
            k1 = k + 1
            h1 = h_ref[pl.ds(j1, 8, stride=0), :]
            f1 = h_ref[pl.ds(NB + j1, 8, stride=0), :]
            acc = [zero] * n_g
            piv = [zero] * n_g
            accn = zero
            alf = zero
            for t in range(n_tiles):
                x = row(out_ref, j, t)
                x1 = row(out_ref, j1, t)
                if t < 2:
                    rid = lane + t * LANES
                    xm = jnp.where(rid > k, x, 0.0)
                    pm = jnp.where(rid == k, 1.0, 0.0)
                    x1 = x1 - h1 * xm - f1 * pm
                    alf = alf + jnp.where(rid == k1, x1, 0.0)
                    x1 = jnp.where(rid > k1, x1, 0.0)
                else:
                    x1 = x1 - h1 * x
                accn = accn + x1 * x1
                for i in range(n_g):
                    a = out_ref[tile(g0 + i, t)]
                    if t < 2:
                        a = a - hs[i] * xm - fs[i] * pm
                        piv[i] = piv[i] + jnp.where(rid == k1, a, 0.0)
                    else:
                        a = a - hs[i] * x
                    out_ref[tile(g0 + i, t)] = a
                    acc[i] = acc[i] + x1 * a
            return finish(acc, piv, accn, alf), coef

        carry, coef = lax.fori_loop(0, 8, step, (carry, [zero] * 3))
        for i in range(3):
            st_ref[i, pl.ds(8 * g0, 8), :] = coef[i]
        dots, pivs, norm2, alpha = carry
        carry = (dots[1:], pivs[1:], norm2, alpha)

    lane16 = lax.broadcasted_iota(jnp.int32, (16, LANES), 1)
    sub16 = lax.broadcasted_iota(jnp.int32, (16, LANES), 0)
    for g in range(groups // 2):
        scale = st_ref[1, pl.ds(16 * g, 16), :]
        beta = st_ref[2, pl.ds(16 * g, 16), :]
        kk = base + 16 * g + sub16
        place = pl.ds(base + 16 * g, 16)
        for t in range(n_tiles):
            a = out_ref[t, place, :]
            v = a * scale
            full = v
            if t < 2:
                rid = lane16 + t * LANES
                full = jnp.where(rid > kk, v, jnp.where(rid == kk, beta, a))
                v = jnp.where(rid > kk, v, jnp.where(rid == kk, 1.0, 0.0))
            out_ref[t, place, :] = full
            for i, part in enumerate(split3(v)):
                vs_ref[i, t, place, :] = part


def panel_dots(load_lhs, rows, panel, vs_ref, acc_ref, n_tiles):
    step_tiles = 8
    acc_ref[pl.ds(0, rows), :] = jnp.zeros((rows, NB), jnp.float32)

    def body(chunk, _):
        parts = [load_lhs(chunk * step_tiles + i) for i in range(step_tiles)]
        lhs = jnp.concatenate([jnp.concatenate([p[s] for p in parts], axis=1) for s in range(3)], axis=0)
        rhs = jnp.concatenate(
            [
                jnp.concatenate(
                    [vs_ref[s, chunk * step_tiles + i, pl.ds(panel * NB, NB), :] for i in range(step_tiles)], axis=1
                )
                for s in range(3)
            ],
            axis=0,
        )
        prod = lax.dot_general(lhs, rhs, (((1,), (1,)), ((), ())), preferred_element_type=jnp.float32)
        top, mid, low = prod[:rows], prod[rows : 2 * rows], prod[2 * rows :]
        small = (top[:, 2 * NB :] + low[:, :NB]) + mid[:, NB : 2 * NB]
        acc_ref[pl.ds(0, rows), :] += (small + (top[:, NB : 2 * NB] + mid[:, :NB])) + top[:, :NB]
        return 0

    lax.fori_loop(0, n_tiles // step_tiles, body, 0)
    return acc_ref[pl.ds(0, rows), :]


def t_from_gram(gram, tau_rows):
    ii = lax.broadcasted_iota(jnp.int32, (NB, NB), 0)
    jj = lax.broadcasted_iota(jnp.int32, (NB, NB), 1)
    eye = jnp.where(ii == jj, 1.0, 0.0)
    power = jnp.where(jj > ii, -tau_rows * gram, 0.0)
    inv = eye + power
    for _ in range(5):
        power = small_dot(power, power)
        inv = inv + small_dot(inv, power)
    tau_cols = jnp.sum(jnp.where(ii == jj, tau_rows, 0.0), axis=0, keepdims=True)
    return inv * tau_cols


def factor_all_kernel(p_ref, out_ref, vs_ref, t_ref, tfull_ref, st_ref, h_ref, acc_ref):
    n_tiles = p_ref.shape[0]
    tfull_ref[...] = jnp.zeros_like(tfull_ref)
    for panel in range(PANELS):
        src = p_ref if panel == 0 else out_ref
        factor_panel(panel, src, out_ref, vs_ref, st_ref, h_ref)
        seen = NB * (panel + 1)
        gram = panel_dots(
            lambda t: [vs_ref[s, t, pl.ds(0, seen), :] for s in range(3)], seen, panel, vs_ref, acc_ref, n_tiles
        )
        t_mat = t_from_gram(gram[seen - NB :], st_ref[0][:, :NB])
        t_ref[panel] = t_mat
        here = pl.ds(seen - NB, NB)
        tfull_ref[here, here] = t_mat
        if panel:
            before = pl.ds(0, seen - NB)
            cross = small_dot(tfull_ref[before, before], gram[: seen - NB])
            tfull_ref[before, here] = -small_dot(cross, t_mat)
        if panel == PANELS - 1:
            break
        left = WIDTH - seen
        rest = pl.ds(seen, left)
        w_sum = panel_dots(lambda t: split3(src[t, rest, :]), left, panel, vs_ref, acc_ref, n_tiles)
        high, mid, low = split3(small_dot(w_sum, t_mat))
        lhs = jnp.concatenate([high, high, high, mid, mid, low], axis=1)

        def body(pair, _):
            tiles = (2 * pair, 2 * pair + 1)
            rhs = jnp.concatenate(
                [
                    jnp.concatenate([vs_ref[s, t, pl.ds(panel * NB, NB), :] for t in tiles], axis=1)
                    for s in (0, 1, 2, 0, 1, 0)
                ],
                axis=0,
            )
            prod = jnp.dot(lhs, rhs, preferred_element_type=jnp.float32)
            for i, t in enumerate(tiles):
                out_ref[t, rest, :] = src[t, rest, :] - prod[:, i * LANES : (i + 1) * LANES]
            return 0

        lax.fori_loop(0, n_tiles // 2, body, 0)


def factor_all(panels):
    n_tiles = panels.shape[0]
    vmem = pl.BlockSpec(memory_space=pltpu.VMEM)
    return pl.pallas_call(
        factor_all_kernel,
        out_shape=(
            jax.ShapeDtypeStruct(panels.shape, jnp.float32),
            jax.ShapeDtypeStruct((3, *panels.shape), jnp.bfloat16),
            jax.ShapeDtypeStruct((PANELS, NB, NB), jnp.float32),
            jax.ShapeDtypeStruct((WIDTH, WIDTH), jnp.float32),
        ),
        in_specs=[vmem],
        out_specs=[vmem] * 4,
        scratch_shapes=[
            pltpu.VMEM((3, NB, LANES), jnp.float32),
            pltpu.VMEM((2 * NB, LANES), jnp.float32),
            pltpu.VMEM((WIDTH, NB), jnp.float32),
        ],
        compiler_params=pltpu.CompilerParams(vmem_limit_bytes=60 * 1024 * 1024),
        name="factor_all",
    )(panels)


PAIR = 2


def refl_tile(packed, first_row):
    rows = first_row + lax.broadcasted_iota(jnp.int32, packed.shape, 1)
    cols = lax.broadcasted_iota(jnp.int32, packed.shape, 0)
    return jnp.where(rows > cols, packed, jnp.where(rows == cols, 1.0, 0.0))


def w_chunk(vt_ref, load_a, local_rows, k_block):
    def body(kb, acc):
        a = load_a(pl.multiple_of(kb * k_block, k_block), k_block)
        high, mid, low = split3(a)
        place = pl.ds(pl.multiple_of(kb * k_block, k_block), k_block)
        full = jnp.dot(vt_ref[:, place], high, preferred_element_type=jnp.float32)
        most = jnp.dot(vt_ref[: 2 * WIDTH, place], mid, preferred_element_type=jnp.float32)
        least = jnp.dot(vt_ref[:WIDTH, place], low, preferred_element_type=jnp.float32)
        small = (full[2 * WIDTH :] + least) + most[WIDTH:]
        return acc + ((small + (full[WIDTH : 2 * WIDTH] + most[:WIDTH])) + full[:WIDTH])

    return lax.fori_loop(0, local_rows // k_block, body, jnp.zeros((WIDTH, PAIR * LANES), jnp.float32))


MESH = pl.DeviceIdType.MESH


def reduce_kernel(a_ref, packed_ref, t_ref, w_ref, pk_buf, vt_ref, a_buf, ws_buf, wr_buf, wm_buf, wx_buf,
                  pk_sem, a_sem, ws_send, ws_recv, wx_send, wx_recv, w2_send, w2_recv):
    local_rows = a_ref.shape[0]
    tiles = local_rows // LANES
    pairs = a_ref.shape[1] // PAIR // 2
    depth = a_buf.shape[0]
    lag = 3
    rank = lax.axis_index('row')
    core = lax.rem(rank, 2)
    partner = rank + 1 - 2 * core
    across = lax.rem(rank + 2, 4)

    barrier = pltpu.get_barrier_semaphore()
    for peer in (partner, across):
        pl.semaphore_signal(barrier, inc=1, device_id={'row': peer}, device_id_type=MESH)

    pk_copy = pltpu.make_async_copy(packed_ref.at[pl.ds(rank * tiles, tiles)], pk_buf, pk_sem)
    pk_copy.start()

    def chunk_of(seq):
        return seq - lax.rem(seq, 2) + lax.rem(seq + 1 + core, 2)

    def fetch(seq, half):
        slot = lax.rem(seq, depth)
        return pltpu.make_async_copy(
            a_ref.at[:, PAIR * chunk_of(seq) + half, :], a_buf.at[slot, half], a_sem.at[slot, half]
        )

    for seq in range(depth):
        for half in range(PAIR):
            fetch(seq, half).start()
    pk_copy.wait()

    def build(t, _):
        v = refl_tile(pk_buf[t], rank * local_rows + t * LANES)
        for s, part in enumerate(split3(v)):
            vt_ref[pl.ds(s * WIDTH, WIDTH), pl.ds(pl.multiple_of(t * LANES, LANES), LANES)] = part
        return 0

    lax.fori_loop(0, tiles, build, 0)
    pl.semaphore_wait(barrier, 2)

    def partial_sum(seq):
        slot = lax.rem(seq, depth)
        for half in range(PAIR):
            fetch(seq, half).wait()
        a = jnp.concatenate([a_buf[slot, half] for half in range(PAIR)], axis=1)
        high, mid, low = split3(a)
        full = jnp.dot(vt_ref[...], high, preferred_element_type=jnp.float32)
        most = jnp.dot(vt_ref[: 2 * WIDTH, :], mid, preferred_element_type=jnp.float32)
        least = jnp.dot(vt_ref[:WIDTH, :], low, preferred_element_type=jnp.float32)
        small = (full[2 * WIDTH :] + least) + most[WIDTH:]
        return (small + (full[WIDTH : 2 * WIDTH] + most[:WIDTH])) + full[:WIDTH]

    def refill(seq):
        @pl.when(seq + depth < 2 * pairs)
        def _():
            for half in range(PAIR):
                fetch(seq + depth, half).start()

    def to_partner(i):
        return pltpu.make_async_remote_copy(
            src_ref=ws_buf.at[lax.rem(i, 2)], dst_ref=wr_buf.at[i], send_sem=ws_send.at[i], recv_sem=ws_recv.at[i],
            device_id={'row': partner}, device_id_type=MESH,
        )

    def to_across(i):
        return pltpu.make_async_remote_copy(
            src_ref=wm_buf.at[i], dst_ref=wx_buf.at[i], send_sem=wx_send.at[i], recv_sem=wx_recv.at[i],
            device_id={'row': across}, device_id_type=MESH,
        )

    def result(i, whose):
        return pltpu.make_async_remote_copy(
            src_ref=w_ref.at[2 * i + whose], dst_ref=w_ref.at[2 * i + whose], send_sem=w2_send.at[i],
            recv_sem=w2_recv.at[i], device_id={'row': partner}, device_id_type=MESH,
        )

    def pair(i, _):
        @pl.when(i < pairs)
        def _():
            theirs = partial_sum(2 * i)

            @pl.when(i >= 2)
            def _():
                to_partner(i - 2).wait_send()

            ws_buf[lax.rem(i, 2)] = theirs
            refill(2 * i)
            to_partner(i).start()
            mine = partial_sum(2 * i + 1)
            refill(2 * i + 1)
            to_partner(i).wait_recv()
            wm_buf[i] = mine + wr_buf[i]
            to_across(i).start()

        @pl.when(i >= lag)
        def _():
            j = i - lag
            to_across(j).wait_recv()
            w_ref[2 * j + core] = lax.dot_general(
                t_ref[...], wm_buf[j] + wx_buf[j], (((0,), (0,)), ((), ())), precision=HIGHEST,
                preferred_element_type=jnp.float32,
            )
            result(j, core).start()

        return 0

    lax.fori_loop(0, pairs + lag, pair, 0)
    for i in (pairs - 2, pairs - 1):
        to_partner(i).wait_send()

    def drain(i, _):
        to_across(i).wait_send()
        result(i, core).wait_send()
        result(i, 1 - core).wait_recv()
        return 0

    lax.fori_loop(0, pairs, drain, 0)


def reduce_w(a3, packed, t_full):
    local_rows, in_block, _ = a3.shape
    tiles = local_rows // LANES
    pairs = in_block // PAIR // 2
    depth = 4
    piece = (WIDTH, PAIR * LANES)
    return pl.pallas_call(
        reduce_kernel,
        out_shape=jax.ShapeDtypeStruct((2 * pairs, *piece), jnp.float32),
        in_specs=[pl.BlockSpec(memory_space=pl.ANY)] * 2 + [pl.BlockSpec(memory_space=pltpu.VMEM)],
        out_specs=pl.BlockSpec(memory_space=pltpu.VMEM),
        scratch_shapes=[
            pltpu.VMEM((tiles, WIDTH, LANES), jnp.float32),
            pltpu.VMEM((3 * WIDTH, local_rows), jnp.bfloat16),
            pltpu.VMEM((depth, PAIR, local_rows, LANES), jnp.float32),
            pltpu.VMEM((2, *piece), jnp.float32),
            pltpu.VMEM((pairs, *piece), jnp.float32),
            pltpu.VMEM((pairs, *piece), jnp.float32),
            pltpu.VMEM((pairs, *piece), jnp.float32),
            pltpu.SemaphoreType.DMA,
            pltpu.SemaphoreType.DMA((depth, PAIR)),
        ] + [pltpu.SemaphoreType.DMA((pairs,))] * 6,
        compiler_params=pltpu.CompilerParams(
            vmem_limit_bytes=56 * 1024 * 1024, collective_id=0, has_side_effects=True
        ),
        name="reduce_w",
    )(a3, packed, t_full)


def apply_kernel(row_rank_fn, col_rank_fn, col_count, a_ref, packed_ref, w_ref, o_ref,
                 pk_buf, vr_ref, pt_ref, a_buf, w_buf, pk_sem, a_sem, w_sem, o_sem):
    local_rows = a_ref.shape[0]
    tiles = local_rows // LANES
    chunks = a_ref.shape[1] // PAIR
    depth = a_buf.shape[0]
    ahead = depth - 2
    own = PANELS // col_count
    row_rank = row_rank_fn()
    col_rank = col_rank_fn()
    pk_copy = pltpu.make_async_copy(packed_ref.at[pl.ds(row_rank * tiles, tiles)], pk_buf, pk_sem)
    pk_copy.start()

    def fetch(i, half):
        slot = lax.rem(i, depth)
        return pltpu.make_async_copy(a_ref.at[:, PAIR * i + half, :], a_buf.at[slot, half], a_sem.at[slot, half])

    def fetch_w(i):
        slot = lax.rem(i, depth)
        return pltpu.make_async_copy(w_ref.at[i], w_buf.at[slot], w_sem.at[slot])

    def put(i, half):
        slot = lax.rem(i, depth)
        return pltpu.make_async_copy(a_buf.at[slot, half], o_ref.at[:, PAIR * i + half, :], o_sem.at[slot, half])

    for i in range(ahead):
        fetch_w(i).start()
        for half in range(PAIR):
            fetch(i, half).start()
    pk_copy.wait()

    def build(t, _):
        place = pl.ds(pl.multiple_of(t * LANES, LANES), LANES)
        packed = pk_buf[t]
        v = refl_tile(packed, row_rank * local_rows + t * LANES).T
        for s, part in enumerate(split3(v)):
            vr_ref[place, s * WIDTH : (s + 1) * WIDTH] = part
        mine = jnp.concatenate(
            [pk_buf[t, pl.ds(pl.multiple_of((b * col_count + col_rank) * NB, NB), NB), :] for b in range(own)], axis=0
        )
        pt_ref[place, :] = mine.T
        return 0

    lax.fori_loop(0, tiles, build, 0)
    m_block = 2048
    lane = lax.broadcasted_iota(jnp.int32, (m_block, LANES), 1)

    def chunk(i, _):
        slot = lax.rem(i, depth)
        fetch_w(i).wait()
        for half in range(PAIR):
            fetch(i, half).wait()
        high, mid, low = split3(w_buf[slot])
        rhs = jnp.concatenate([high, mid, low, high, mid, high], axis=0)

        def body(mb, _):
            rows = pl.ds(pl.multiple_of(mb * m_block, m_block), m_block)
            vh, vm, vl = (vr_ref[rows, s * WIDTH : (s + 1) * WIDTH] for s in range(3))
            lhs = jnp.concatenate([vh, vh, vh, vm, vm, vl], axis=1)
            prod = jnp.dot(lhs, rhs, preferred_element_type=jnp.float32)
            done = pt_ref[rows, :]
            for half in range(PAIR):
                new = a_buf[slot, half, rows, :] - prod[:, half * LANES : (half + 1) * LANES]
                for b in range(own):
                    shift = lax.rem(2 * LANES + b - b * NB - (PAIR * i + half), LANES)
                    new = jnp.where(lane == b, pltpu.roll(done, shift, 1), new)
                a_buf[slot, half, rows, :] = new
            return 0

        lax.fori_loop(0, local_rows // m_block, body, 0)
        for half in range(PAIR):
            put(i, half).start()

        @pl.when(i + ahead < chunks)
        def _():
            @pl.when(i + ahead >= depth)
            def _():
                for half in range(PAIR):
                    put(i + ahead - depth, half).wait()

            fetch_w(i + ahead).start()
            for half in range(PAIR):
                fetch(i + ahead, half).start()

        return 0

    lax.fori_loop(0, chunks, chunk, 0)
    for i in range(chunks - depth, chunks):
        for half in range(PAIR):
            put(i, half).wait()


def apply_local(a3, packed, w, row_rank_fn, col_rank_fn, col_count):
    local_rows, in_block, _ = a3.shape
    tiles = local_rows // LANES
    depth = 5
    return pl.pallas_call(
        lambda *refs: apply_kernel(row_rank_fn, col_rank_fn, col_count, *refs),
        out_shape=jax.ShapeDtypeStruct(a3.shape, jnp.float32),
        in_specs=[pl.BlockSpec(memory_space=pl.ANY)] * 3,
        out_specs=pl.BlockSpec(memory_space=pl.ANY),
        scratch_shapes=[
            pltpu.VMEM((tiles, WIDTH, LANES), jnp.float32),
            pltpu.VMEM((local_rows, 3 * WIDTH), jnp.bfloat16),
            pltpu.VMEM((local_rows, LANES), jnp.float32),
            pltpu.VMEM((depth, PAIR, local_rows, LANES), jnp.float32),
            pltpu.VMEM((depth, WIDTH, PAIR * LANES), jnp.float32),
            pltpu.SemaphoreType.DMA,
            pltpu.SemaphoreType.DMA((depth, PAIR)),
            pltpu.SemaphoreType.DMA((depth,)),
            pltpu.SemaphoreType.DMA((depth, PAIR)),
        ],
        compiler_params=pltpu.CompilerParams(vmem_limit_bytes=56 * 1024 * 1024),
        name="apply_local",
    )(a3, packed, w)


def solution(mesh):
    col_count = mesh.shape['col']
    block_spec = P(('batch', 'row'), 'col', None)
    own = PANELS // col_count

    def device_fn(a_local):
        local_rows, _, _ = a_local.shape
        local_tiles = local_rows // LANES
        share = a_local[:, :own, :].reshape(local_tiles, LANES, own, NB).transpose(2, 0, 3, 1)
        every = lax.all_gather(lax.all_gather(share, 'row'), 'col')
        panels = every.transpose(1, 3, 2, 0, 4, 5).reshape(-1, WIDTH, LANES)
        packed, _, t_factors, t_full = factor_all(panels)
        a3 = a_local.transpose(0, 2, 1)
        w_mat = reduce_w(a3, packed, t_full)
        a_new = apply_local(a3, packed, w_mat, lambda: lax.axis_index('row'), lambda: lax.axis_index('col'), col_count)
        tau = jnp.diagonal(t_factors, axis1=1, axis2=2).reshape(-1)
        return a_new.transpose(0, 2, 1), tau, t_factors

    return jax.shard_map(device_fn, mesh=mesh, in_specs=(block_spec,), out_specs=(block_spec, P('batch'), P('batch', None, None)), check_vma=False)
```

```python
import jax
import jax.numpy as jnp
from jax import lax
from jax.experimental import pallas as pl
from jax.experimental.pallas import tpu as pltpu
from jax.sharding import PartitionSpec as P

NB = 64
LANES = 128
PANELS = 4
WIDTH = NB * PANELS
HIGHEST = lax.Precision.HIGHEST


def split3(x):
    high = x.astype(jnp.bfloat16)
    rest = x - high.astype(jnp.float32)
    mid = rest.astype(jnp.bfloat16)
    low = (rest - mid.astype(jnp.float32)).astype(jnp.bfloat16)
    return high, mid, low


def small_dot(a, b):
    return jnp.dot(a, b, precision=HIGHEST, preferred_element_type=jnp.float32)


def factor_panel(panel, src_ref, out_ref, vs_ref, st_ref, h_ref):
    n_tiles = src_ref.shape[0]
    base = panel * NB
    lane = lax.broadcasted_iota(jnp.int32, (8, LANES), 1)
    sub = lax.broadcasted_iota(jnp.int32, (8, LANES), 0)
    groups = NB // 8
    zero = jnp.zeros((8, LANES), jnp.float32)

    def tile(g, t):
        return (t, pl.ds(base + 8 * g, 8), slice(None))

    def splat(v):
        return jnp.broadcast_to(jnp.sum(v, axis=1, keepdims=True), (8, LANES))

    def row(ref, j, t):
        return ref[t, pl.ds(base + j, 8, stride=0), :]

    def finish(acc, piv, accn, alf):
        return [splat(a) for a in acc], [splat(a) for a in piv], splat(accn), splat(alf)

    def start():
        acc = [zero] * groups
        piv = [zero] * groups
        accn = zero
        alf = zero
        for t in range(n_tiles):
            x = row(src_ref, 0, t)
            if t < 2:
                rid = lane + t * LANES
                alf = alf + jnp.where(rid == base, x, 0.0)
                x = jnp.where(rid > base, x, 0.0)
            accn = accn + x * x
            for g in range(groups):
                a = src_ref[tile(g, t)]
                if src_ref is not out_ref:
                    out_ref[tile(g, t)] = a
                if t < 2:
                    piv[g] = piv[g] + jnp.where(rid == base, a, 0.0)
                acc[g] = acc[g] + x * a
        return finish(acc, piv, accn, alf)

    carry = start()
    for g0 in range(groups):
        n_g = groups - g0

        def step(s, carry, g0=g0, n_g=n_g):
            (dots, pivs, norm2, alpha), coef = carry
            j = g0 * 8 + s
            k = base + j
            norm = jnp.sqrt(alpha * alpha + norm2)
            beta = jnp.where(alpha >= 0.0, -norm, norm)
            tau = (beta - alpha) / beta
            scale = 1.0 / (alpha - beta)
            coef = [jnp.where(sub == s, new, old) for new, old in zip((tau, scale, beta), coef)]
            hs, fs = [], []
            for i in range(n_g):
                f = tau * (scale * dots[i] + pivs[i])
                if i == 0:
                    f = jnp.where(sub > s, f, 0.0)
                h = f * scale
                h_ref[pl.ds(8 * (g0 + i), 8), :] = h
                h_ref[pl.ds(NB + 8 * (g0 + i), 8), :] = f
                hs.append(h)
                fs.append(f)
            j1 = jnp.minimum(j + 1, NB - 1)
            k1 = k + 1
            h1 = h_ref[pl.ds(j1, 8, stride=0), :]
            f1 = h_ref[pl.ds(NB + j1, 8, stride=0), :]
            acc = [zero] * n_g
            piv = [zero] * n_g
            accn = zero
            alf = zero
            for t in range(n_tiles):
                x = row(out_ref, j, t)
                x1 = row(out_ref, j1, t)
                if t < 2:
                    rid = lane + t * LANES
                    xm = jnp.where(rid > k, x, 0.0)
                    pm = jnp.where(rid == k, 1.0, 0.0)
                    x1 = x1 - h1 * xm - f1 * pm
                    alf = alf + jnp.where(rid == k1, x1, 0.0)
                    x1 = jnp.where(rid > k1, x1, 0.0)
                else:
                    x1 = x1 - h1 * x
                accn = accn + x1 * x1
                for i in range(n_g):
                    a = out_ref[tile(g0 + i, t)]
                    if t < 2:
                        a = a - hs[i] * xm - fs[i] * pm
                        piv[i] = piv[i] + jnp.where(rid == k1, a, 0.0)
                    else:
                        a = a - hs[i] * x
                    out_ref[tile(g0 + i, t)] = a
                    acc[i] = acc[i] + x1 * a
            return finish(acc, piv, accn, alf), coef

        carry, coef = lax.fori_loop(0, 8, step, (carry, [zero] * 3))
        for i in range(3):
            st_ref[i, pl.ds(8 * g0, 8), :] = coef[i]
        dots, pivs, norm2, alpha = carry
        carry = (dots[1:], pivs[1:], norm2, alpha)

    lane16 = lax.broadcasted_iota(jnp.int32, (16, LANES), 1)
    sub16 = lax.broadcasted_iota(jnp.int32, (16, LANES), 0)
    for g in range(groups // 2):
        scale = st_ref[1, pl.ds(16 * g, 16), :]
        beta = st_ref[2, pl.ds(16 * g, 16), :]
        kk = base + 16 * g + sub16
        place = pl.ds(base + 16 * g, 16)
        for t in range(n_tiles):
            a = out_ref[t, place, :]
            v = a * scale
            full = v
            if t < 2:
                rid = lane16 + t * LANES
                full = jnp.where(rid > kk, v, jnp.where(rid == kk, beta, a))
                v = jnp.where(rid > kk, v, jnp.where(rid == kk, 1.0, 0.0))
            out_ref[t, place, :] = full
            for i, part in enumerate(split3(v)):
                vs_ref[i, t, place, :] = part


def panel_dots(load_lhs, rows, panel, vs_ref, acc_ref, n_tiles):
    step_tiles = 8
    acc_ref[pl.ds(0, rows), :] = jnp.zeros((rows, NB), jnp.float32)

    def body(chunk, _):
        parts = [load_lhs(chunk * step_tiles + i) for i in range(step_tiles)]
        lhs = jnp.concatenate([jnp.concatenate([p[s] for p in parts], axis=1) for s in range(3)], axis=0)
        rhs = jnp.concatenate(
            [
                jnp.concatenate(
                    [vs_ref[s, chunk * step_tiles + i, pl.ds(panel * NB, NB), :] for i in range(step_tiles)], axis=1
                )
                for s in range(3)
            ],
            axis=0,
        )
        prod = lax.dot_general(lhs, rhs, (((1,), (1,)), ((), ())), preferred_element_type=jnp.float32)
        top, mid, low = prod[:rows], prod[rows : 2 * rows], prod[2 * rows :]
        small = (top[:, 2 * NB :] + low[:, :NB]) + mid[:, NB : 2 * NB]
        acc_ref[pl.ds(0, rows), :] += (small + (top[:, NB : 2 * NB] + mid[:, :NB])) + top[:, :NB]
        return 0

    lax.fori_loop(0, n_tiles // step_tiles, body, 0)
    return acc_ref[pl.ds(0, rows), :]


def t_from_gram(gram, tau_rows):
    ii = lax.broadcasted_iota(jnp.int32, (NB, NB), 0)
    jj = lax.broadcasted_iota(jnp.int32, (NB, NB), 1)
    eye = jnp.where(ii == jj, 1.0, 0.0)
    power = jnp.where(jj > ii, -tau_rows * gram, 0.0)
    inv = eye + power
    for _ in range(5):
        power = small_dot(power, power)
        inv = inv + small_dot(inv, power)
    tau_cols = jnp.sum(jnp.where(ii == jj, tau_rows, 0.0), axis=0, keepdims=True)
    return inv * tau_cols


def factor_all_kernel(p_ref, out_ref, vs_ref, t_ref, tfull_ref, st_ref, h_ref, acc_ref):
    n_tiles = p_ref.shape[0]
    tfull_ref[...] = jnp.zeros_like(tfull_ref)
    for panel in range(PANELS):
        src = p_ref if panel == 0 else out_ref
        factor_panel(panel, src, out_ref, vs_ref, st_ref, h_ref)
        seen = NB * (panel + 1)
        gram = panel_dots(
            lambda t: [vs_ref[s, t, pl.ds(0, seen), :] for s in range(3)], seen, panel, vs_ref, acc_ref, n_tiles
        )
        t_mat = t_from_gram(gram[seen - NB :], st_ref[0][:, :NB])
        t_ref[panel] = t_mat
        here = pl.ds(seen - NB, NB)
        tfull_ref[here, here] = t_mat
        if panel:
            before = pl.ds(0, seen - NB)
            cross = small_dot(tfull_ref[before, before], gram[: seen - NB])
            tfull_ref[before, here] = -small_dot(cross, t_mat)
        if panel == PANELS - 1:
            break
        left = WIDTH - seen
        rest = pl.ds(seen, left)
        w_sum = panel_dots(lambda t: split3(src[t, rest, :]), left, panel, vs_ref, acc_ref, n_tiles)
        high, mid, low = split3(small_dot(w_sum, t_mat))
        lhs = jnp.concatenate([high, high, high, mid, mid, low], axis=1)

        def body(pair, _):
            tiles = (2 * pair, 2 * pair + 1)
            rhs = jnp.concatenate(
                [
                    jnp.concatenate([vs_ref[s, t, pl.ds(panel * NB, NB), :] for t in tiles], axis=1)
                    for s in (0, 1, 2, 0, 1, 0)
                ],
                axis=0,
            )
            prod = jnp.dot(lhs, rhs, preferred_element_type=jnp.float32)
            for i, t in enumerate(tiles):
                out_ref[t, rest, :] = src[t, rest, :] - prod[:, i * LANES : (i + 1) * LANES]
            return 0

        lax.fori_loop(0, n_tiles // 2, body, 0)


def factor_all(panels):
    n_tiles = panels.shape[0]
    vmem = pl.BlockSpec(memory_space=pltpu.VMEM)
    return pl.pallas_call(
        factor_all_kernel,
        out_shape=(
            jax.ShapeDtypeStruct(panels.shape, jnp.float32),
            jax.ShapeDtypeStruct((3, *panels.shape), jnp.bfloat16),
            jax.ShapeDtypeStruct((PANELS, NB, NB), jnp.float32),
            jax.ShapeDtypeStruct((WIDTH, WIDTH), jnp.float32),
        ),
        in_specs=[vmem],
        out_specs=[vmem] * 4,
        scratch_shapes=[
            pltpu.VMEM((3, NB, LANES), jnp.float32),
            pltpu.VMEM((2 * NB, LANES), jnp.float32),
            pltpu.VMEM((WIDTH, NB), jnp.float32),
        ],
        compiler_params=pltpu.CompilerParams(vmem_limit_bytes=60 * 1024 * 1024),
        name="factor_all",
    )(panels)


PAIR = 2


def refl_tile(packed, first_row):
    rows = first_row + lax.broadcasted_iota(jnp.int32, packed.shape, 1)
    cols = lax.broadcasted_iota(jnp.int32, packed.shape, 0)
    return jnp.where(rows > cols, packed, jnp.where(rows == cols, 1.0, 0.0))


def w_chunk(vt_ref, load_a, local_rows, k_block):
    def body(kb, acc):
        a = load_a(pl.multiple_of(kb * k_block, k_block), k_block)
        high, mid, low = split3(a)
        place = pl.ds(pl.multiple_of(kb * k_block, k_block), k_block)
        full = jnp.dot(vt_ref[:, place], high, preferred_element_type=jnp.float32)
        most = jnp.dot(vt_ref[: 2 * WIDTH, place], mid, preferred_element_type=jnp.float32)
        least = jnp.dot(vt_ref[:WIDTH, place], low, preferred_element_type=jnp.float32)
        small = (full[2 * WIDTH :] + least) + most[WIDTH:]
        return acc + ((small + (full[WIDTH : 2 * WIDTH] + most[:WIDTH])) + full[:WIDTH])

    return lax.fori_loop(0, local_rows // k_block, body, jnp.zeros((WIDTH, PAIR * LANES), jnp.float32))


MESH = pl.DeviceIdType.MESH


def reduce_kernel(a_ref, packed_ref, t_ref, w_ref, pk_buf, vt_ref, a_buf, ws_buf, wr_buf, wm_buf, wx_buf,
                  pk_sem, a_sem, ws_send, ws_recv, wx_send, wx_recv, w2_send, w2_recv):
    local_rows = a_ref.shape[0]
    tiles = local_rows // LANES
    pairs = a_ref.shape[1] // PAIR // 2
    depth = a_buf.shape[0]
    lag = 3
    rank = lax.axis_index('row')
    core = lax.rem(rank, 2)
    partner = rank + 1 - 2 * core
    across = lax.rem(rank + 2, 4)

    barrier = pltpu.get_barrier_semaphore()
    for peer in (partner, across):
        pl.semaphore_signal(barrier, inc=1, device_id={'row': peer}, device_id_type=MESH)

    pk_copy = pltpu.make_async_copy(packed_ref.at[pl.ds(rank * tiles, tiles)], pk_buf, pk_sem)
    pk_copy.start()

    def chunk_of(seq):
        return seq - lax.rem(seq, 2) + lax.rem(seq + 1 + core, 2)

    def fetch(seq, half):
        slot = lax.rem(seq, depth)
        return pltpu.make_async_copy(
            a_ref.at[:, PAIR * chunk_of(seq) + half, :], a_buf.at[slot, half], a_sem.at[slot, half]
        )

    for seq in range(depth):
        for half in range(PAIR):
            fetch(seq, half).start()
    pk_copy.wait()

    def build(t, _):
        v = refl_tile(pk_buf[t], rank * local_rows + t * LANES)
        for s, part in enumerate(split3(v)):
            vt_ref[pl.ds(s * WIDTH, WIDTH), pl.ds(pl.multiple_of(t * LANES, LANES), LANES)] = part
        return 0

    lax.fori_loop(0, tiles, build, 0)
    pl.semaphore_wait(barrier, 2)

    def partial_sum(seq):
        slot = lax.rem(seq, depth)
        for half in range(PAIR):
            fetch(seq, half).wait()
        a = jnp.concatenate([a_buf[slot, half] for half in range(PAIR)], axis=1)
        high, mid, low = split3(a)
        full = jnp.dot(vt_ref[...], high, preferred_element_type=jnp.float32)
        most = jnp.dot(vt_ref[: 2 * WIDTH, :], mid, preferred_element_type=jnp.float32)
        least = jnp.dot(vt_ref[:WIDTH, :], low, preferred_element_type=jnp.float32)
        small = (full[2 * WIDTH :] + least) + most[WIDTH:]
        return (small + (full[WIDTH : 2 * WIDTH] + most[:WIDTH])) + full[:WIDTH]

    def refill(seq):
        @pl.when(seq + depth < 2 * pairs)
        def _():
            for half in range(PAIR):
                fetch(seq + depth, half).start()

    def to_partner(i):
        return pltpu.make_async_remote_copy(
            src_ref=ws_buf.at[lax.rem(i, 2)], dst_ref=wr_buf.at[i], send_sem=ws_send.at[i], recv_sem=ws_recv.at[i],
            device_id={'row': partner}, device_id_type=MESH,
        )

    def to_across(i):
        return pltpu.make_async_remote_copy(
            src_ref=wm_buf.at[i], dst_ref=wx_buf.at[i], send_sem=wx_send.at[i], recv_sem=wx_recv.at[i],
            device_id={'row': across}, device_id_type=MESH,
        )

    def result(i, whose):
        return pltpu.make_async_remote_copy(
            src_ref=w_ref.at[2 * i + whose], dst_ref=w_ref.at[2 * i + whose], send_sem=w2_send.at[i],
            recv_sem=w2_recv.at[i], device_id={'row': partner}, device_id_type=MESH,
        )

    def pair(i, _):
        @pl.when(i < pairs)
        def _():
            theirs = partial_sum(2 * i)

            @pl.when(i >= 2)
            def _():
                to_partner(i - 2).wait_send()

            ws_buf[lax.rem(i, 2)] = theirs
            refill(2 * i)
            to_partner(i).start()
            mine = partial_sum(2 * i + 1)
            refill(2 * i + 1)
            to_partner(i).wait_recv()
            wm_buf[i] = mine + wr_buf[i]
            to_across(i).start()

        @pl.when(i >= lag)
        def _():
            j = i - lag
            to_across(j).wait_recv()
            w_ref[2 * j + core] = lax.dot_general(
                t_ref[...], wm_buf[j] + wx_buf[j], (((0,), (0,)), ((), ())), precision=HIGHEST,
                preferred_element_type=jnp.float32,
            )
            result(j, core).start()

        return 0

    lax.fori_loop(0, pairs + lag, pair, 0)
    for i in (pairs - 2, pairs - 1):
        to_partner(i).wait_send()

    def drain(i, _):
        to_across(i).wait_send()
        result(i, core).wait_send()
        result(i, 1 - core).wait_recv()
        return 0

    lax.fori_loop(0, pairs, drain, 0)


def reduce_w(a3, packed, t_full):
    local_rows, in_block, _ = a3.shape
    tiles = local_rows // LANES
    pairs = in_block // PAIR // 2
    depth = 4
    piece = (WIDTH, PAIR * LANES)
    return pl.pallas_call(
        reduce_kernel,
        out_shape=jax.ShapeDtypeStruct((2 * pairs, *piece), jnp.float32),
        in_specs=[pl.BlockSpec(memory_space=pl.ANY)] * 2 + [pl.BlockSpec(memory_space=pltpu.VMEM)],
        out_specs=pl.BlockSpec(memory_space=pltpu.VMEM),
        scratch_shapes=[
            pltpu.VMEM((tiles, WIDTH, LANES), jnp.float32),
            pltpu.VMEM((3 * WIDTH, local_rows), jnp.bfloat16),
            pltpu.VMEM((depth, PAIR, local_rows, LANES), jnp.float32),
            pltpu.VMEM((2, *piece), jnp.float32),
            pltpu.VMEM((pairs, *piece), jnp.float32),
            pltpu.VMEM((pairs, *piece), jnp.float32),
            pltpu.VMEM((pairs, *piece), jnp.float32),
            pltpu.SemaphoreType.DMA,
            pltpu.SemaphoreType.DMA((depth, PAIR)),
        ] + [pltpu.SemaphoreType.DMA((pairs,))] * 6,
        compiler_params=pltpu.CompilerParams(
            vmem_limit_bytes=56 * 1024 * 1024, collective_id=0, has_side_effects=True
        ),
        name="reduce_w",
    )(a3, packed, t_full)


def gather_kernel(own, col_count, a_ref, out_ref, a_buf, a_sem, d_send, d_recv, x_send, x_recv, y_send, y_recv):
    local_rows, in_block, _ = a_ref.shape
    tiles = local_rows // LANES
    depth = a_buf.shape[0]
    pieces = x_send.shape[1]
    piece_tiles = tiles // pieces
    rank = lax.axis_index('row')
    col = lax.axis_index('col')
    core = lax.rem(rank, 2)
    partner = rank + 1 - 2 * core
    across = lax.rem(rank + 2, 4)
    beside = 1 - col

    barrier = pltpu.get_barrier_semaphore()
    for peer in ({'row': partner}, {'row': across}, {'col': beside}):
        pl.semaphore_signal(barrier, inc=1, device_id=peer, device_id_type=MESH)

    def fetch(t):
        slot = lax.rem(t, depth)
        return pltpu.make_async_copy(a_ref.at[pl.ds(t * LANES, LANES)], a_buf.at[slot], a_sem.at[slot])

    for t in range(depth):
        fetch(t).start()

    lane = lax.broadcasted_iota(jnp.int32, (8, LANES), 1)

    def extract(t, _):
        fetch(t).wait()
        slot = lax.rem(t, depth)

        def group(g, _):
            outs = [jnp.zeros((8, LANES), jnp.float32)] * own
            for r in range(LANES):
                x = a_buf[slot, r, pl.ds(pl.multiple_of(8 * g, 8), 8), :]
                outs = [
                    jnp.where(lane == r, pltpu.roll(x, (r - b) % LANES, 1) if r != b else x, outs[b])
                    for b in range(own)
                ]
            for b in range(own):
                first = pl.multiple_of((b * col_count + col) * NB + 8 * g, 8)
                out_ref[rank * tiles + t, pl.ds(first, 8), :] = outs[b]
            return 0

        lax.fori_loop(0, in_block // 8, group, 0)

        @pl.when(t + depth < tiles)
        def _():
            fetch(t + depth).start()

        return 0

    def copy(row, column, b, piece, send, recv, peer):
        where = out_ref.at[
            pl.ds(row * tiles + piece * piece_tiles, piece_tiles),
            pl.ds(pl.multiple_of((b * col_count + column) * NB, NB), NB),
            :,
        ]
        return pltpu.make_async_remote_copy(
            src_ref=where, dst_ref=where, send_sem=send, recv_sem=recv, device_id=peer, device_id_type=MESH
        )

    origins = ((rank, col), (across, col), (rank, beside), (across, beside))
    across_p = lax.rem(partner + 2, 4)
    origins_p = ((partner, col), (across_p, col), (partner, beside), (across_p, beside))

    def to_partner(kind, b, piece, sending=True):
        origin = (origins if sending else origins_p)[kind]
        return copy(*origin, b, piece, d_send.at[kind, b, piece], d_recv.at[kind, b, piece], {'row': partner})

    def over_x(kind, b, piece, sending=True):
        origin = ((rank, col) if kind == 0 else (rank, beside)) if sending else ((across, col) if kind == 0 else (across, beside))
        return copy(*origin, b, piece, x_send.at[kind * own + b, piece], x_recv.at[kind * own + b, piece], {'row': across})

    def over_y(kind, b, piece, sending=True):
        origin = ((rank, col) if kind == 0 else (across, col)) if sending else ((rank, beside) if kind == 0 else (across, beside))
        return copy(*origin, b, piece, y_send.at[kind * own + b, piece], y_recv.at[kind * own + b, piece], {'col': beside})

    def spread(piece):
        for b in range(own):
            over_x(0, b, piece).start()
            over_y(0, b, piece).start()
            to_partner(0, b, piece).start()

    def forward(piece):
        for b in range(own):
            over_x(0, b, piece, False).wait_recv()
            if b % 2:
                over_y(1, b, piece).start()
            to_partner(1, b, piece).start()
            over_y(0, b, piece, False).wait_recv()
            if b % 2 == 0:
                over_x(1, b, piece).start()
            to_partner(2, b, piece).start()

    def last(piece):
        for b in range(own):
            (over_y if b % 2 else over_x)(1, b, piece, False).wait_recv()
            to_partner(3, b, piece).start()

    for piece in range(pieces):
        lax.fori_loop(piece * piece_tiles, (piece + 1) * piece_tiles, extract, 0)
        if piece == 0:
            pl.semaphore_wait(barrier, 3)
        spread(piece)
        if piece:
            forward(piece - 1)
    forward(pieces - 1)
    for piece in range(pieces):
        last(piece)
    for piece in range(pieces):
        for b in range(own):
            for kind in range(4):
                to_partner(kind, b, piece).wait_send()
                to_partner(kind, b, piece, False).wait_recv()
            over_x(0, b, piece).wait_send()
            over_y(0, b, piece).wait_send()
            (over_y if b % 2 else over_x)(1, b, piece).wait_send()


def gather_panels(a3, own, col_count, row_count):
    local_rows, in_block, lanes = a3.shape
    tiles = local_rows // LANES
    depth = 3
    pieces = 4
    d_sems = pltpu.SemaphoreType.DMA((4, own, pieces))
    link_sems = pltpu.SemaphoreType.DMA((2 * own, pieces))
    return pl.pallas_call(
        lambda *refs: gather_kernel(own, col_count, *refs),
        out_shape=jax.ShapeDtypeStruct((row_count * tiles, WIDTH, LANES), jnp.float32),
        in_specs=[pl.BlockSpec(memory_space=pl.ANY)],
        out_specs=pl.BlockSpec(memory_space=pltpu.VMEM),
        scratch_shapes=[
            pltpu.VMEM((depth, LANES, in_block, lanes), jnp.float32),
            pltpu.SemaphoreType.DMA((depth,)),
            d_sems, d_sems, link_sems, link_sems, link_sems, link_sems,
        ],
        compiler_params=pltpu.CompilerParams(
            vmem_limit_bytes=40 * 1024 * 1024, collective_id=1, has_side_effects=True
        ),
        name="gather_panels",
    )(a3)


def apply_kernel(row_rank_fn, col_rank_fn, col_count, a_ref, packed_ref, w_ref, o_ref,
                 pk_buf, vr_ref, pt_ref, a_buf, w_buf, pk_sem, a_sem, w_sem, o_sem):
    local_rows = a_ref.shape[0]
    tiles = local_rows // LANES
    chunks = a_ref.shape[1] // PAIR
    depth = a_buf.shape[0]
    ahead = depth - 2
    own = PANELS // col_count
    row_rank = row_rank_fn()
    col_rank = col_rank_fn()
    pk_copy = pltpu.make_async_copy(packed_ref.at[pl.ds(row_rank * tiles, tiles)], pk_buf, pk_sem)
    pk_copy.start()

    def fetch(i, half):
        slot = lax.rem(i, depth)
        return pltpu.make_async_copy(a_ref.at[:, PAIR * i + half, :], a_buf.at[slot, half], a_sem.at[slot, half])

    def fetch_w(i):
        slot = lax.rem(i, depth)
        return pltpu.make_async_copy(w_ref.at[i], w_buf.at[slot], w_sem.at[slot])

    def put(i, half):
        slot = lax.rem(i, depth)
        return pltpu.make_async_copy(a_buf.at[slot, half], o_ref.at[:, PAIR * i + half, :], o_sem.at[slot, half])

    for i in range(ahead):
        fetch_w(i).start()
        for half in range(PAIR):
            fetch(i, half).start()
    pk_copy.wait()

    def build(t, _):
        place = pl.ds(pl.multiple_of(t * LANES, LANES), LANES)
        packed = pk_buf[t]
        v = refl_tile(packed, row_rank * local_rows + t * LANES).T
        for s, part in enumerate(split3(v)):
            vr_ref[place, s * WIDTH : (s + 1) * WIDTH] = part
        mine = jnp.concatenate(
            [pk_buf[t, pl.ds(pl.multiple_of((b * col_count + col_rank) * NB, NB), NB), :] for b in range(own)], axis=0
        )
        pt_ref[place, :] = mine.T
        return 0

    lax.fori_loop(0, tiles, build, 0)
    m_block = 2048
    lane = lax.broadcasted_iota(jnp.int32, (m_block, LANES), 1)

    def chunk(i, _):
        slot = lax.rem(i, depth)
        fetch_w(i).wait()
        for half in range(PAIR):
            fetch(i, half).wait()
        high, mid, low = split3(w_buf[slot])
        rhs = jnp.concatenate([high, mid, low, high, mid, high], axis=0)

        def body(mb, _):
            rows = pl.ds(pl.multiple_of(mb * m_block, m_block), m_block)
            vh, vm, vl = (vr_ref[rows, s * WIDTH : (s + 1) * WIDTH] for s in range(3))
            lhs = jnp.concatenate([vh, vh, vh, vm, vm, vl], axis=1)
            prod = jnp.dot(lhs, rhs, preferred_element_type=jnp.float32)
            done = pt_ref[rows, :]
            for half in range(PAIR):
                new = a_buf[slot, half, rows, :] - prod[:, half * LANES : (half + 1) * LANES]
                for b in range(own):
                    shift = lax.rem(2 * LANES + b - b * NB - (PAIR * i + half), LANES)
                    new = jnp.where(lane == b, pltpu.roll(done, shift, 1), new)
                a_buf[slot, half, rows, :] = new
            return 0

        lax.fori_loop(0, local_rows // m_block, body, 0)
        for half in range(PAIR):
            put(i, half).start()

        @pl.when(i + ahead < chunks)
        def _():
            @pl.when(i + ahead >= depth)
            def _():
                for half in range(PAIR):
                    put(i + ahead - depth, half).wait()

            fetch_w(i + ahead).start()
            for half in range(PAIR):
                fetch(i + ahead, half).start()

        return 0

    lax.fori_loop(0, chunks, chunk, 0)
    for i in range(chunks - depth, chunks):
        for half in range(PAIR):
            put(i, half).wait()


def apply_local(a3, packed, w, row_rank_fn, col_rank_fn, col_count):
    local_rows, in_block, _ = a3.shape
    tiles = local_rows // LANES
    depth = 5
    return pl.pallas_call(
        lambda *refs: apply_kernel(row_rank_fn, col_rank_fn, col_count, *refs),
        out_shape=jax.ShapeDtypeStruct(a3.shape, jnp.float32),
        in_specs=[pl.BlockSpec(memory_space=pl.ANY)] * 3,
        out_specs=pl.BlockSpec(memory_space=pl.ANY),
        scratch_shapes=[
            pltpu.VMEM((tiles, WIDTH, LANES), jnp.float32),
            pltpu.VMEM((local_rows, 3 * WIDTH), jnp.bfloat16),
            pltpu.VMEM((local_rows, LANES), jnp.float32),
            pltpu.VMEM((depth, PAIR, local_rows, LANES), jnp.float32),
            pltpu.VMEM((depth, WIDTH, PAIR * LANES), jnp.float32),
            pltpu.SemaphoreType.DMA,
            pltpu.SemaphoreType.DMA((depth, PAIR)),
            pltpu.SemaphoreType.DMA((depth,)),
            pltpu.SemaphoreType.DMA((depth, PAIR)),
        ],
        compiler_params=pltpu.CompilerParams(vmem_limit_bytes=56 * 1024 * 1024),
        name="apply_local",
    )(a3, packed, w)


def solution(mesh):
    col_count = mesh.shape['col']
    block_spec = P(('batch', 'row'), 'col', None)
    own = PANELS // col_count

    def device_fn(a_local):
        a3 = a_local.transpose(0, 2, 1)
        panels = gather_panels(a3, own, col_count, mesh.shape['row'])
        packed, _, t_factors, t_full = factor_all(panels)
        w_mat = reduce_w(a3, packed, t_full)
        a_new = apply_local(a3, packed, w_mat, lambda: lax.axis_index('row'), lambda: lax.axis_index('col'), col_count)
        tau = jnp.diagonal(t_factors, axis1=1, axis2=2).reshape(-1)
        return a_new.transpose(0, 2, 1), tau, t_factors

    return jax.shard_map(device_fn, mesh=mesh, in_specs=(block_spec,), out_specs=(block_spec, P('batch'), P('batch', None, None)), check_vma=False)
```

```python
import jax
import jax.numpy as jnp
from jax import lax
from jax.experimental import pallas as pl
from jax.experimental.pallas import tpu as pltpu
from jax.sharding import PartitionSpec as P

NB = 64
UNROLL = 31
LANES = 128
PANELS = 4
WIDTH = NB * PANELS
HIGHEST = lax.Precision.HIGHEST


def split3(x):
    high = x.astype(jnp.bfloat16)
    rest = x - high.astype(jnp.float32)
    mid = rest.astype(jnp.bfloat16)
    low = (rest - mid.astype(jnp.float32)).astype(jnp.bfloat16)
    return high, mid, low


def small_dot(a, b):
    return jnp.dot(a, b, precision=HIGHEST, preferred_element_type=jnp.float32)


def factor_panel(panel, src_ref, out_ref, vs_ref, st_ref, h_ref):
    n_tiles = src_ref.shape[0]
    base = panel * NB
    lane = lax.broadcasted_iota(jnp.int32, (8, LANES), 1)
    sub = lax.broadcasted_iota(jnp.int32, (8, LANES), 0)
    groups = NB // 8
    zero = jnp.zeros((8, LANES), jnp.float32)

    def tile(g, t):
        return (t, pl.ds(base + 8 * g, 8), slice(None))

    def splat(v):
        return jnp.broadcast_to(jnp.sum(v, axis=1, keepdims=True), (8, LANES))

    def row(ref, j, t):
        return ref[t, pl.ds(base + j, 8, stride=0), :]

    def finish(acc, piv, accn, alf):
        return [splat(a) for a in acc], [splat(a) for a in piv], splat(accn), splat(alf)

    def start():
        acc = [zero] * groups
        piv = [zero] * groups
        accn = zero
        alf = zero
        for t in range(n_tiles):
            x = row(src_ref, 0, t)
            if t < 2:
                rid = lane + t * LANES
                alf = alf + jnp.where(rid == base, x, 0.0)
                x = jnp.where(rid > base, x, 0.0)
            accn = accn + x * x
            for g in range(groups):
                a = src_ref[tile(g, t)]
                if src_ref is not out_ref:
                    out_ref[tile(g, t)] = a
                if t < 2:
                    piv[g] = piv[g] + jnp.where(rid == base, a, 0.0)
                acc[g] = acc[g] + x * a
        return finish(acc, piv, accn, alf)

    carry = start()
    for g0 in range(groups):
        n_g = groups - g0

        def step(s, carry, g0=g0, n_g=n_g):
            (dots, pivs, norm2, alpha), coef = carry
            j = g0 * 8 + s
            k = base + j
            norm = jnp.sqrt(alpha * alpha + norm2)
            beta = jnp.where(alpha >= 0.0, -norm, norm)
            tau = (beta - alpha) / beta
            scale = 1.0 / (alpha - beta)
            coef = [jnp.where(sub == s, new, old) for new, old in zip((tau, scale, beta), coef)]
            hs, fs = [], []
            for i in range(n_g):
                f = tau * (scale * dots[i] + pivs[i])
                if i == 0:
                    f = jnp.where(sub > s, f, 0.0)
                h = f * scale
                h_ref[pl.ds(8 * (g0 + i), 8), :] = h
                h_ref[pl.ds(NB + 8 * (g0 + i), 8), :] = f
                hs.append(h)
                fs.append(f)
            j1 = jnp.minimum(j + 1, NB - 1)
            k1 = k + 1
            h1 = h_ref[pl.ds(j1, 8, stride=0), :]
            f1 = h_ref[pl.ds(NB + j1, 8, stride=0), :]
            acc = [zero] * n_g
            piv = [zero] * n_g
            accn = zero
            alf = zero
            for t in range(2):
                x = row(out_ref, j, t)
                x1 = row(out_ref, j1, t)
                rid = lane + t * LANES
                xm = jnp.where(rid > k, x, 0.0)
                pm = jnp.where(rid == k, 1.0, 0.0)
                x1 = x1 - h1 * xm - f1 * pm
                alf = alf + jnp.where(rid == k1, x1, 0.0)
                x1 = jnp.where(rid > k1, x1, 0.0)
                accn = accn + x1 * x1
                for i in range(n_g):
                    a = out_ref[tile(g0 + i, t)]
                    a = a - hs[i] * xm - fs[i] * pm
                    piv[i] = piv[i] + jnp.where(rid == k1, a, 0.0)
                    out_ref[tile(g0 + i, t)] = a
                    acc[i] = acc[i] + x1 * a

            def some(c, sums):
                accn, acc = sums
                acc = list(acc)
                for u in range(UNROLL):
                    t = 2 + c * UNROLL + u
                    x = row(out_ref, j, t)
                    x1 = row(out_ref, j1, t) - h1 * x
                    accn = accn + x1 * x1
                    for i in range(n_g):
                        a = out_ref[tile(g0 + i, t)] - hs[i] * x
                        out_ref[tile(g0 + i, t)] = a
                        acc[i] = acc[i] + x1 * a
                return accn, acc

            accn, acc = lax.fori_loop(0, (n_tiles - 2) // UNROLL, some, (accn, acc))
            return finish(acc, piv, accn, alf), coef

        carry, coef = lax.fori_loop(0, 8, step, (carry, [zero] * 3))
        for i in range(3):
            st_ref[i, pl.ds(8 * g0, 8), :] = coef[i]
        dots, pivs, norm2, alpha = carry
        carry = (dots[1:], pivs[1:], norm2, alpha)

    lane16 = lax.broadcasted_iota(jnp.int32, (16, LANES), 1)
    sub16 = lax.broadcasted_iota(jnp.int32, (16, LANES), 0)
    for g in range(groups // 2):
        scale = st_ref[1, pl.ds(16 * g, 16), :]
        beta = st_ref[2, pl.ds(16 * g, 16), :]
        kk = base + 16 * g + sub16
        place = pl.ds(base + 16 * g, 16)
        for t in range(n_tiles):
            a = out_ref[t, place, :]
            v = a * scale
            full = v
            if t < 2:
                rid = lane16 + t * LANES
                full = jnp.where(rid > kk, v, jnp.where(rid == kk, beta, a))
                v = jnp.where(rid > kk, v, jnp.where(rid == kk, 1.0, 0.0))
            out_ref[t, place, :] = full
            for i, part in enumerate(split3(v)):
                vs_ref[i, t, place, :] = part


def panel_dots(load_lhs, rows, panel, vs_ref, acc_ref, n_tiles):
    step_tiles = 8
    acc_ref[pl.ds(0, rows), :] = jnp.zeros((rows, NB), jnp.float32)

    def body(chunk, _):
        parts = [load_lhs(chunk * step_tiles + i) for i in range(step_tiles)]
        lhs = jnp.concatenate([jnp.concatenate([p[s] for p in parts], axis=1) for s in range(3)], axis=0)
        rhs = jnp.concatenate(
            [
                jnp.concatenate(
                    [vs_ref[s, chunk * step_tiles + i, pl.ds(panel * NB, NB), :] for i in range(step_tiles)], axis=1
                )
                for s in range(3)
            ],
            axis=0,
        )
        prod = lax.dot_general(lhs, rhs, (((1,), (1,)), ((), ())), preferred_element_type=jnp.float32)
        top, mid, low = prod[:rows], prod[rows : 2 * rows], prod[2 * rows :]
        small = (top[:, 2 * NB :] + low[:, :NB]) + mid[:, NB : 2 * NB]
        acc_ref[pl.ds(0, rows), :] += (small + (top[:, NB : 2 * NB] + mid[:, :NB])) + top[:, :NB]
        return 0

    lax.fori_loop(0, n_tiles // step_tiles, body, 0)
    return acc_ref[pl.ds(0, rows), :]


def t_from_gram(gram, tau_rows):
    ii = lax.broadcasted_iota(jnp.int32, (NB, NB), 0)
    jj = lax.broadcasted_iota(jnp.int32, (NB, NB), 1)
    eye = jnp.where(ii == jj, 1.0, 0.0)
    power = jnp.where(jj > ii, -tau_rows * gram, 0.0)
    inv = eye + power
    for _ in range(5):
        power = small_dot(power, power)
        inv = inv + small_dot(inv, power)
    tau_cols = jnp.sum(jnp.where(ii == jj, tau_rows, 0.0), axis=0, keepdims=True)
    return inv * tau_cols


def factor_all_kernel(p_ref, out_ref, vs_ref, t_ref, tfull_ref, st_ref, h_ref, acc_ref):
    n_tiles = p_ref.shape[0]
    tfull_ref[...] = jnp.zeros_like(tfull_ref)
    for panel in range(PANELS):
        src = p_ref if panel == 0 else out_ref
        factor_panel(panel, src, out_ref, vs_ref, st_ref, h_ref)
        seen = NB * (panel + 1)
        gram = panel_dots(
            lambda t: [vs_ref[s, t, pl.ds(0, seen), :] for s in range(3)], seen, panel, vs_ref, acc_ref, n_tiles
        )
        t_mat = t_from_gram(gram[seen - NB :], st_ref[0][:, :NB])
        t_ref[panel] = t_mat
        here = pl.ds(seen - NB, NB)
        tfull_ref[here, here] = t_mat
        if panel:
            before = pl.ds(0, seen - NB)
            cross = small_dot(tfull_ref[before, before], gram[: seen - NB])
            tfull_ref[before, here] = -small_dot(cross, t_mat)
        if panel == PANELS - 1:
            break
        left = WIDTH - seen
        rest = pl.ds(seen, left)
        w_sum = panel_dots(lambda t: split3(src[t, rest, :]), left, panel, vs_ref, acc_ref, n_tiles)
        high, mid, low = split3(small_dot(w_sum, t_mat))
        lhs = jnp.concatenate([high, high, high, mid, mid, low], axis=1)

        def body(pair, _):
            tiles = (2 * pair, 2 * pair + 1)
            rhs = jnp.concatenate(
                [
                    jnp.concatenate([vs_ref[s, t, pl.ds(panel * NB, NB), :] for t in tiles], axis=1)
                    for s in (0, 1, 2, 0, 1, 0)
                ],
                axis=0,
            )
            prod = jnp.dot(lhs, rhs, preferred_element_type=jnp.float32)
            for i, t in enumerate(tiles):
                out_ref[t, rest, :] = src[t, rest, :] - prod[:, i * LANES : (i + 1) * LANES]
            return 0

        lax.fori_loop(0, n_tiles // 2, body, 0)


def factor_all(panels):
    n_tiles = panels.shape[0]
    vmem = pl.BlockSpec(memory_space=pltpu.VMEM)
    return pl.pallas_call(
        factor_all_kernel,
        out_shape=(
            jax.ShapeDtypeStruct(panels.shape, jnp.float32),
            jax.ShapeDtypeStruct((3, *panels.shape), jnp.bfloat16),
            jax.ShapeDtypeStruct((PANELS, NB, NB), jnp.float32),
            jax.ShapeDtypeStruct((WIDTH, WIDTH), jnp.float32),
        ),
        in_specs=[vmem],
        out_specs=[vmem] * 4,
        scratch_shapes=[
            pltpu.VMEM((3, NB, LANES), jnp.float32),
            pltpu.VMEM((2 * NB, LANES), jnp.float32),
            pltpu.VMEM((WIDTH, NB), jnp.float32),
        ],
        compiler_params=pltpu.CompilerParams(vmem_limit_bytes=60 * 1024 * 1024),
        name="factor_all",
    )(panels)


PAIR = 2


def refl_tile(packed, first_row):
    rows = first_row + lax.broadcasted_iota(jnp.int32, packed.shape, 1)
    cols = lax.broadcasted_iota(jnp.int32, packed.shape, 0)
    return jnp.where(rows > cols, packed, jnp.where(rows == cols, 1.0, 0.0))


def w_chunk(vt_ref, load_a, local_rows, k_block):
    def body(kb, acc):
        a = load_a(pl.multiple_of(kb * k_block, k_block), k_block)
        high, mid, low = split3(a)
        place = pl.ds(pl.multiple_of(kb * k_block, k_block), k_block)
        full = jnp.dot(vt_ref[:, place], high, preferred_element_type=jnp.float32)
        most = jnp.dot(vt_ref[: 2 * WIDTH, place], mid, preferred_element_type=jnp.float32)
        least = jnp.dot(vt_ref[:WIDTH, place], low, preferred_element_type=jnp.float32)
        small = (full[2 * WIDTH :] + least) + most[WIDTH:]
        return acc + ((small + (full[WIDTH : 2 * WIDTH] + most[:WIDTH])) + full[:WIDTH])

    return lax.fori_loop(0, local_rows // k_block, body, jnp.zeros((WIDTH, PAIR * LANES), jnp.float32))


MESH = pl.DeviceIdType.MESH


def reduce_kernel(a_ref, packed_ref, t_ref, w_ref, pk_buf, vt_ref, a_buf, ws_buf, wr_buf, wm_buf, wx_buf,
                  pk_sem, a_sem, ws_send, ws_recv, wx_send, wx_recv, w2_send, w2_recv):
    local_rows = a_ref.shape[0]
    tiles = local_rows // LANES
    pairs = a_ref.shape[1] // PAIR // 2
    depth = a_buf.shape[0]
    lag = 3
    rank = lax.axis_index('row')
    core = lax.rem(rank, 2)
    partner = rank + 1 - 2 * core
    across = lax.rem(rank + 2, 4)

    barrier = pltpu.get_barrier_semaphore()
    for peer in (partner, across):
        pl.semaphore_signal(barrier, inc=1, device_id={'row': peer}, device_id_type=MESH)

    pk_copy = pltpu.make_async_copy(packed_ref.at[pl.ds(rank * tiles, tiles)], pk_buf, pk_sem)
    pk_copy.start()

    def chunk_of(seq):
        return seq - lax.rem(seq, 2) + lax.rem(seq + 1 + core, 2)

    def fetch(seq, half):
        slot = lax.rem(seq, depth)
        return pltpu.make_async_copy(
            a_ref.at[:, PAIR * chunk_of(seq) + half, :], a_buf.at[slot, half], a_sem.at[slot, half]
        )

    for seq in range(depth):
        for half in range(PAIR):
            fetch(seq, half).start()
    pk_copy.wait()

    def build(t, _):
        v = refl_tile(pk_buf[t], rank * local_rows + t * LANES)
        for s, part in enumerate(split3(v)):
            vt_ref[pl.ds(s * WIDTH, WIDTH), pl.ds(pl.multiple_of(t * LANES, LANES), LANES)] = part
        return 0

    lax.fori_loop(0, tiles, build, 0)
    pl.semaphore_wait(barrier, 2)

    def partial_sum(seq):
        slot = lax.rem(seq, depth)
        for half in range(PAIR):
            fetch(seq, half).wait()
        a = jnp.concatenate([a_buf[slot, half] for half in range(PAIR)], axis=1)
        high, mid, low = split3(a)
        full = jnp.dot(vt_ref[...], high, preferred_element_type=jnp.float32)
        most = jnp.dot(vt_ref[: 2 * WIDTH, :], mid, preferred_element_type=jnp.float32)
        least = jnp.dot(vt_ref[:WIDTH, :], low, preferred_element_type=jnp.float32)
        small = (full[2 * WIDTH :] + least) + most[WIDTH:]
        return (small + (full[WIDTH : 2 * WIDTH] + most[:WIDTH])) + full[:WIDTH]

    def refill(seq):
        @pl.when(seq + depth < 2 * pairs)
        def _():
            for half in range(PAIR):
                fetch(seq + depth, half).start()

    def to_partner(i):
        return pltpu.make_async_remote_copy(
            src_ref=ws_buf.at[lax.rem(i, 2)], dst_ref=wr_buf.at[i], send_sem=ws_send.at[i], recv_sem=ws_recv.at[i],
            device_id={'row': partner}, device_id_type=MESH,
        )

    def to_across(i):
        return pltpu.make_async_remote_copy(
            src_ref=wm_buf.at[i], dst_ref=wx_buf.at[i], send_sem=wx_send.at[i], recv_sem=wx_recv.at[i],
            device_id={'row': across}, device_id_type=MESH,
        )

    def result(i, whose):
        return pltpu.make_async_remote_copy(
            src_ref=w_ref.at[2 * i + whose], dst_ref=w_ref.at[2 * i + whose], send_sem=w2_send.at[i],
            recv_sem=w2_recv.at[i], device_id={'row': partner}, device_id_type=MESH,
        )

    def step(seq, _):
        i = seq // 2
        first = lax.rem(seq, 2) == 0

        @pl.when(seq < 2 * pairs)
        def _():
            part = partial_sum(seq)
            refill(seq)

            @pl.when(first)
            def _():
                @pl.when(i >= 2)
                def _():
                    to_partner(i - 2).wait_send()

                ws_buf[lax.rem(i, 2)] = part
                to_partner(i).start()

            @pl.when(jnp.logical_not(first))
            def _():
                to_partner(i).wait_recv()
                wm_buf[i] = part + wr_buf[i]
                to_across(i).start()

        @pl.when(jnp.logical_not(first) & (i >= lag))
        def _():
            j = i - lag
            to_across(j).wait_recv()
            w_ref[2 * j + core] = lax.dot_general(
                t_ref[...], wm_buf[j] + wx_buf[j], (((0,), (0,)), ((), ())), precision=HIGHEST,
                preferred_element_type=jnp.float32,
            )
            result(j, core).start()

        return 0

    lax.fori_loop(0, 2 * (pairs + lag), step, 0)
    for i in (pairs - 2, pairs - 1):
        to_partner(i).wait_send()

    def drain(i, _):
        to_across(i).wait_send()
        result(i, core).wait_send()
        result(i, 1 - core).wait_recv()
        return 0

    lax.fori_loop(0, pairs, drain, 0)


def reduce_w(a3, packed, t_full):
    local_rows, in_block, _ = a3.shape
    tiles = local_rows // LANES
    pairs = in_block // PAIR // 2
    depth = 4
    piece = (WIDTH, PAIR * LANES)
    return pl.pallas_call(
        reduce_kernel,
        out_shape=jax.ShapeDtypeStruct((2 * pairs, *piece), jnp.float32),
        in_specs=[pl.BlockSpec(memory_space=pl.ANY)] * 2 + [pl.BlockSpec(memory_space=pltpu.VMEM)],
        out_specs=pl.BlockSpec(memory_space=pltpu.VMEM),
        scratch_shapes=[
            pltpu.VMEM((tiles, WIDTH, LANES), jnp.float32),
            pltpu.VMEM((3 * WIDTH, local_rows), jnp.bfloat16),
            pltpu.VMEM((depth, PAIR, local_rows, LANES), jnp.float32),
            pltpu.VMEM((2, *piece), jnp.float32),
            pltpu.VMEM((pairs, *piece), jnp.float32),
            pltpu.VMEM((pairs, *piece), jnp.float32),
            pltpu.VMEM((pairs, *piece), jnp.float32),
            pltpu.SemaphoreType.DMA,
            pltpu.SemaphoreType.DMA((depth, PAIR)),
        ] + [pltpu.SemaphoreType.DMA((pairs,))] * 6,
        compiler_params=pltpu.CompilerParams(
            vmem_limit_bytes=56 * 1024 * 1024, collective_id=0, has_side_effects=True
        ),
        name="reduce_w",
    )(a3, packed, t_full)


def gather_kernel(own, col_count, a_ref, out_ref, a_buf, a_sem, d_send, d_recv, x_send, x_recv, y_send, y_recv):
    local_rows, in_block, _ = a_ref.shape
    tiles = local_rows // LANES
    depth = a_buf.shape[0]
    pieces = x_send.shape[1]
    piece_tiles = tiles // pieces
    rank = lax.axis_index('row')
    col = lax.axis_index('col')
    core = lax.rem(rank, 2)
    partner = rank + 1 - 2 * core
    across = lax.rem(rank + 2, 4)
    beside = 1 - col

    barrier = pltpu.get_barrier_semaphore()
    for peer in ({'row': partner}, {'row': across}, {'col': beside}):
        pl.semaphore_signal(barrier, inc=1, device_id=peer, device_id_type=MESH)

    def fetch(t):
        slot = lax.rem(t, depth)
        return pltpu.make_async_copy(a_ref.at[pl.ds(t * LANES, LANES)], a_buf.at[slot], a_sem.at[slot])

    for t in range(depth):
        fetch(t).start()

    lane = lax.broadcasted_iota(jnp.int32, (8, LANES), 1)

    def extract(t, _):
        fetch(t).wait()
        slot = lax.rem(t, depth)

        def group(g, _):
            outs = [jnp.zeros((8, LANES), jnp.float32)] * own
            for r in range(LANES):
                x = a_buf[slot, r, pl.ds(pl.multiple_of(8 * g, 8), 8), :]
                outs = [
                    jnp.where(lane == r, pltpu.roll(x, (r - b) % LANES, 1) if r != b else x, outs[b])
                    for b in range(own)
                ]
            for b in range(own):
                first = pl.multiple_of((b * col_count + col) * NB + 8 * g, 8)
                out_ref[rank * tiles + t, pl.ds(first, 8), :] = outs[b]
            return 0

        lax.fori_loop(0, in_block // 8, group, 0)

        @pl.when(t + depth < tiles)
        def _():
            fetch(t + depth).start()

        return 0

    def copy(row, column, b, piece, send, recv, peer):
        where = out_ref.at[
            pl.ds(row * tiles + piece * piece_tiles, piece_tiles),
            pl.ds(pl.multiple_of((b * col_count + column) * NB, NB), NB),
            :,
        ]
        return pltpu.make_async_remote_copy(
            src_ref=where, dst_ref=where, send_sem=send, recv_sem=recv, device_id=peer, device_id_type=MESH
        )

    origins = ((rank, col), (across, col), (rank, beside), (across, beside))
    across_p = lax.rem(partner + 2, 4)
    origins_p = ((partner, col), (across_p, col), (partner, beside), (across_p, beside))

    def to_partner(kind, b, piece, sending=True):
        origin = (origins if sending else origins_p)[kind]
        return copy(*origin, b, piece, d_send.at[kind, b, piece], d_recv.at[kind, b, piece], {'row': partner})

    def over_x(kind, b, piece, sending=True):
        origin = ((rank, col) if kind == 0 else (rank, beside)) if sending else ((across, col) if kind == 0 else (across, beside))
        return copy(*origin, b, piece, x_send.at[kind * own + b, piece], x_recv.at[kind * own + b, piece], {'row': across})

    def over_y(kind, b, piece, sending=True):
        origin = ((rank, col) if kind == 0 else (across, col)) if sending else ((rank, beside) if kind == 0 else (across, beside))
        return copy(*origin, b, piece, y_send.at[kind * own + b, piece], y_recv.at[kind * own + b, piece], {'col': beside})

    def spread(piece):
        for b in range(own):
            over_x(0, b, piece).start()
            over_y(0, b, piece).start()
            to_partner(0, b, piece).start()

    def forward(piece):
        for b in range(own):
            over_x(0, b, piece, False).wait_recv()
            if b % 2:
                over_y(1, b, piece).start()
            to_partner(1, b, piece).start()
            over_y(0, b, piece, False).wait_recv()
            if b % 2 == 0:
                over_x(1, b, piece).start()
            to_partner(2, b, piece).start()

    def last(piece):
        for b in range(own):
            (over_y if b % 2 else over_x)(1, b, piece, False).wait_recv()
            to_partner(3, b, piece).start()

    for piece in range(pieces):
        lax.fori_loop(piece * piece_tiles, (piece + 1) * piece_tiles, extract, 0)
        if piece == 0:
            pl.semaphore_wait(barrier, 3)
        spread(piece)
        if piece:
            forward(piece - 1)
    forward(pieces - 1)
    for piece in range(pieces):
        last(piece)
    for piece in range(pieces):
        for b in range(own):
            for kind in range(4):
                to_partner(kind, b, piece).wait_send()
                to_partner(kind, b, piece, False).wait_recv()
            over_x(0, b, piece).wait_send()
            over_y(0, b, piece).wait_send()
            (over_y if b % 2 else over_x)(1, b, piece).wait_send()


def gather_panels(a3, own, col_count, row_count):
    local_rows, in_block, lanes = a3.shape
    tiles = local_rows // LANES
    depth = 3
    pieces = 8
    d_sems = pltpu.SemaphoreType.DMA((4, own, pieces))
    link_sems = pltpu.SemaphoreType.DMA((2 * own, pieces))
    return pl.pallas_call(
        lambda *refs: gather_kernel(own, col_count, *refs),
        out_shape=jax.ShapeDtypeStruct((row_count * tiles, WIDTH, LANES), jnp.float32),
        in_specs=[pl.BlockSpec(memory_space=pl.ANY)],
        out_specs=pl.BlockSpec(memory_space=pltpu.VMEM),
        scratch_shapes=[
            pltpu.VMEM((depth, LANES, in_block, lanes), jnp.float32),
            pltpu.SemaphoreType.DMA((depth,)),
            d_sems, d_sems, link_sems, link_sems, link_sems, link_sems,
        ],
        compiler_params=pltpu.CompilerParams(
            vmem_limit_bytes=40 * 1024 * 1024, collective_id=1, has_side_effects=True
        ),
        name="gather_panels",
    )(a3)


def apply_kernel(row_rank_fn, col_rank_fn, col_count, a_ref, packed_ref, w_ref, o_ref,
                 pk_buf, vr_ref, pt_ref, a_buf, w_buf, pk_sem, a_sem, w_sem, o_sem):
    local_rows = a_ref.shape[0]
    tiles = local_rows // LANES
    chunks = a_ref.shape[1] // PAIR
    depth = a_buf.shape[0]
    ahead = depth - 2
    own = PANELS // col_count
    row_rank = row_rank_fn()
    col_rank = col_rank_fn()
    pk_copy = pltpu.make_async_copy(packed_ref.at[pl.ds(row_rank * tiles, tiles)], pk_buf, pk_sem)
    pk_copy.start()

    def fetch(i, half):
        slot = lax.rem(i, depth)
        return pltpu.make_async_copy(a_ref.at[:, PAIR * i + half, :], a_buf.at[slot, half], a_sem.at[slot, half])

    def fetch_w(i):
        slot = lax.rem(i, depth)
        return pltpu.make_async_copy(w_ref.at[i], w_buf.at[slot], w_sem.at[slot])

    def put(i, half):
        slot = lax.rem(i, depth)
        return pltpu.make_async_copy(a_buf.at[slot, half], o_ref.at[:, PAIR * i + half, :], o_sem.at[slot, half])

    for i in range(ahead):
        fetch_w(i).start()
        for half in range(PAIR):
            fetch(i, half).start()
    pk_copy.wait()

    def build(t, _):
        place = pl.ds(pl.multiple_of(t * LANES, LANES), LANES)
        packed = pk_buf[t]
        v = refl_tile(packed, row_rank * local_rows + t * LANES).T
        for s, part in enumerate(split3(v)):
            vr_ref[place, s * WIDTH : (s + 1) * WIDTH] = part
        mine = jnp.concatenate(
            [pk_buf[t, pl.ds(pl.multiple_of((b * col_count + col_rank) * NB, NB), NB), :] for b in range(own)], axis=0
        )
        pt_ref[place, :] = mine.T
        return 0

    lax.fori_loop(0, tiles, build, 0)
    m_block = 2048
    lane = lax.broadcasted_iota(jnp.int32, (m_block, LANES), 1)

    def chunk(i, _):
        slot = lax.rem(i, depth)
        fetch_w(i).wait()
        for half in range(PAIR):
            fetch(i, half).wait()
        high, mid, low = split3(w_buf[slot])
        rhs = jnp.concatenate([high, mid, low, high, mid, high], axis=0)

        def body(mb, _):
            rows = pl.ds(pl.multiple_of(mb * m_block, m_block), m_block)
            vh, vm, vl = (vr_ref[rows, s * WIDTH : (s + 1) * WIDTH] for s in range(3))
            lhs = jnp.concatenate([vh, vh, vh, vm, vm, vl], axis=1)
            prod = jnp.dot(lhs, rhs, preferred_element_type=jnp.float32)
            done = pt_ref[rows, :]
            for half in range(PAIR):
                new = a_buf[slot, half, rows, :] - prod[:, half * LANES : (half + 1) * LANES]
                for b in range(own):
                    shift = lax.rem(2 * LANES + b - b * NB - (PAIR * i + half), LANES)
                    new = jnp.where(lane == b, pltpu.roll(done, shift, 1), new)
                a_buf[slot, half, rows, :] = new
            return 0

        lax.fori_loop(0, local_rows // m_block, body, 0)
        for half in range(PAIR):
            put(i, half).start()

        @pl.when(i + ahead < chunks)
        def _():
            @pl.when(i + ahead >= depth)
            def _():
                for half in range(PAIR):
                    put(i + ahead - depth, half).wait()

            fetch_w(i + ahead).start()
            for half in range(PAIR):
                fetch(i + ahead, half).start()

        return 0

    lax.fori_loop(0, chunks, chunk, 0)
    for i in range(chunks - depth, chunks):
        for half in range(PAIR):
            put(i, half).wait()


def apply_local(a3, packed, w, row_rank_fn, col_rank_fn, col_count):
    local_rows, in_block, _ = a3.shape
    tiles = local_rows // LANES
    depth = 5
    return pl.pallas_call(
        lambda *refs: apply_kernel(row_rank_fn, col_rank_fn, col_count, *refs),
        out_shape=jax.ShapeDtypeStruct(a3.shape, jnp.float32),
        in_specs=[pl.BlockSpec(memory_space=pl.ANY)] * 3,
        out_specs=pl.BlockSpec(memory_space=pl.ANY),
        scratch_shapes=[
            pltpu.VMEM((tiles, WIDTH, LANES), jnp.float32),
            pltpu.VMEM((local_rows, 3 * WIDTH), jnp.bfloat16),
            pltpu.VMEM((local_rows, LANES), jnp.float32),
            pltpu.VMEM((depth, PAIR, local_rows, LANES), jnp.float32),
            pltpu.VMEM((depth, WIDTH, PAIR * LANES), jnp.float32),
            pltpu.SemaphoreType.DMA,
            pltpu.SemaphoreType.DMA((depth, PAIR)),
            pltpu.SemaphoreType.DMA((depth,)),
            pltpu.SemaphoreType.DMA((depth, PAIR)),
        ],
        compiler_params=pltpu.CompilerParams(vmem_limit_bytes=56 * 1024 * 1024),
        name="apply_local",
    )(a3, packed, w)


def solution(mesh):
    col_count = mesh.shape['col']
    block_spec = P(('batch', 'row'), 'col', None)
    own = PANELS // col_count

    def device_fn(a_local):
        a3 = a_local.transpose(0, 2, 1)
        panels = gather_panels(a3, own, col_count, mesh.shape['row'])
        packed, _, t_factors, t_full = factor_all(panels)
        w_mat = reduce_w(a3, packed, t_full)
        a_new = apply_local(a3, packed, w_mat, lambda: lax.axis_index('row'), lambda: lax.axis_index('col'), col_count)
        tau = jnp.diagonal(t_factors, axis1=1, axis2=2).reshape(-1)
        return a_new.transpose(0, 2, 1), tau, t_factors

    return jax.shard_map(device_fn, mesh=mesh, in_specs=(block_spec,), out_specs=(block_spec, P('batch'), P('batch', None, None)), check_vma=False)
```
